256 devices in a mesh: tab: 16 (over z_lo, x), cand: 4 (over z_hi, core), dp: 4 (over y).
Axes of the slice: x: 4, y: 4, z: 8 (z_hi: 2, z_lo: 4; z = z_hi * 4 + z_lo), core: 2. Of those that a mesh axis runs over, the one named last changes fastest.
Arguments:
- tables: bfloat16 [16, 524288, 128], P(('cand', 'dp'), 'tab'), may hold values from -6 to 6
- bag_ids: int32 [16, 1024, 16], P(('cand', 'dp')), may hold values from 0 to 524287
- bag_lengths: int32 [16, 1024], P(('cand', 'dp')), may hold values from 1 to 16
- item_weight: bfloat16 [2048, 256], replicated, may hold values from -0.125 to 0.125
- user_features: bfloat16 [131072, 512], P(('tab', 'dp')), may hold values from -6 to 6
- user_w1: bfloat16 [512, 1024], replicated, may hold values from -0.25 to 0.25
- user_w2: bfloat16 [1024, 256], replicated, may hold values from -0.1875 to 0.1875
- positive_items: int32 [131072], P(('tab', 'dp')), may hold values from 0 to 1023
Outputs:
- item_emb: float32 [1024, 256], P(('tab', 'cand', 'dp'))
- user_loss: float32 [131072], P(('tab', 'dp'))
The draws below stay inside these ranges and needn't reach their ends.
Inputs may be any that keep to these rules, and one draw needn't show every extreme that they name: `bag_ids`: row ids of a table. Only the first bag_lengths ids of a bag count; the rest is padding.
All inputs are finite; a program needn't handle non-finite values.
Results may differ from the reference program's by a relative error of at most 0.00046.
Values sent between devices are 32-bit elements; how exact they have to be, the bound alone decides.
A program may use at most 64 MiB of HBM per device.

```python
import jax
import jax.numpy as jnp
from jax import lax

E = 128
H = 256
DU = 512
HU = 1024
L = 16
ITEMS = 1024
F = 16
VOCAB = 524288
USERS = 131072


def place_ends(array, stream_key, least, top_value):
    place = [jax.random.randint(jax.random.fold_in(stream_key, axis), (), 0, length) for axis, length in enumerate(array.shape)]
    main_axis = array.shape.index(max(array.shape))
    next_to = place[:main_axis] + [(place[main_axis] + 1) % array.shape[main_axis]] + place[main_axis + 1:]
    return array.at[tuple(place)].set(least).at[tuple(next_to)].set(top_value)


def levels(own_key, shape, pieces, least, largest):
    factor_of, own = 1.0, jax.random.fold_in(own_key, 6)
    for position, parts in pieces:
        heights = jnp.exp(jax.random.uniform(jax.random.fold_in(own, position), (parts,), jnp.float32, least / len(pieces), largest / len(pieces)))
        factor_of = factor_of * jnp.repeat(heights, shape[position] // parts).reshape([-1 if axis == position else 1 for axis in range(len(shape))])
    return factor_of


def noise(stream_key, extent, spread, limit, split=(), held_as=jnp.bfloat16):
    gain = levels(stream_key, extent, split, -0.22, 0.18) if split else 1.0
    result = jax.random.normal(stream_key, extent, jnp.float32) * spread * gain
    return jnp.minimum(jnp.maximum(result, -limit), limit).astype(held_as)


def setup_inputs(seed: int = 0) -> dict:
    splits = jax.random.split(jax.random.key(seed), 9)
    return {
        "tables": noise(splits[0], (F, VOCAB, E), 1.0, 6.0, ((0, 16), (1, 16))),
        "bag_ids": place_ends(jax.random.randint(splits[1], (F, ITEMS, L), 0, VOCAB), jax.random.fold_in(splits[1], 1), 0, VOCAB - 1).astype(jnp.int32),
        "bag_lengths": place_ends(jax.random.randint(splits[2], (F, ITEMS), 1, L + 1), jax.random.fold_in(splits[2], 1), 1, L).astype(jnp.int32),
        "item_weight": noise(splits[3], (F * E, H), (F * E) ** -0.5, 0.125),
        "user_features": noise(splits[4], (USERS, DU), 1.0, 6.0, ((0, 64),)),
        "user_w1": noise(splits[5], (DU, HU), DU ** -0.5, 0.25),
        "user_w2": noise(splits[6], (HU, H), HU ** -0.5, 0.1875),
        "positive_items": place_ends(jax.random.randint(splits[7], (USERS,), 0, ITEMS), jax.random.fold_in(splits[7], 1), 0, ITEMS - 1).astype(jnp.int32),
    }


epsilon = 1e-06
logit_scale = 20.0

def unit_rows(vectors):
    return vectors * lax.rsqrt(lax.optimization_barrier(jnp.mean(vectors * vectors, axis=-1, keepdims=True)) + epsilon)

def pool_table(inputs):
    table, bag_ids, lengths = inputs
    gathered = jnp.take(table, bag_ids, axis=0).astype(jnp.float32)
    valid = lax.broadcasted_iota(jnp.int32, bag_ids.shape, 1) < lengths[:, None]
    summed = lax.optimization_barrier(jnp.sum(jnp.where(valid[:, :, None], gathered, jnp.float32(0.0)), axis=1))
    return summed / lengths[:, None].astype(jnp.float32)

def reference(tables, bag_ids, bag_lengths, item_weight, user_features, user_w1, user_w2, positive_items):
    pooled = lax.map(pool_table, (tables, bag_ids, bag_lengths))
    joined = jnp.transpose(pooled, (1, 0, 2)).reshape(ITEMS, F * E)
    item_pre = jnp.dot(joined, item_weight.astype(jnp.float32), precision=lax.Precision.HIGHEST, preferred_element_type=jnp.float32)
    item_emb = unit_rows(item_pre)
    user_hidden = jax.nn.gelu(jnp.dot(user_features, user_w1, preferred_element_type=jnp.float32), approximate=False).astype(jnp.bfloat16)
    user_pre = jnp.dot(user_hidden, user_w2, preferred_element_type=jnp.float32)
    user_emb = unit_rows(user_pre)
    scores = jnp.dot(user_emb, item_emb.T, precision=lax.Precision.HIGHEST, preferred_element_type=jnp.float32) * (logit_scale / H)
    totals = lax.optimization_barrier(jnp.sum(jnp.exp(scores), axis=1))
    positive = jnp.take_along_axis(scores, positive_items[:, None].astype(jnp.int32), axis=1)[:, 0]
    user_loss = jnp.log(totals) - positive
    return (item_emb, user_loss)
```

```python
import functools
import jax
import jax.numpy as jnp
from jax import lax
from jax.experimental import pallas as pl
from jax.experimental.pallas import tpu as pltpu
from jax.sharding import PartitionSpec as P

MESH = pl.DeviceIdType.MESH
f32, bf16, i32 = jnp.float32, jnp.bfloat16, jnp.int32
epsilon = 1e-06
logit_scale = 20.0
NX, NZ = 4, 4
PARTS = 4
DEPTH = 16
CHUNKS = 8


def iota(shape, dim):
    return lax.broadcasted_iota(i32, shape, dim)


def pool_kernel(ids_ref, len_ref, table_ref, out_ref, stage, tab, acc0, acc1, acc2, acc3,
                rank_ref, code_ref, list_ref, slist, load_sems, list_sem):
    rows = table_ref.shape[0]
    positions, items = ids_ref.shape
    tiles = items // 128
    chunk = rows // CHUNKS
    base = lax.axis_index("tab") * rows
    loads = [
        pltpu.make_async_copy(
            table_ref.at[pl.ds(c * chunk, chunk)], stage.at[pl.ds(c * chunk, chunk)], load_sems.at[c]
        )
        for c in range(CHUNKS)
    ]
    for load in loads:
        load.start()
    accs = (acc0, acc1, acc2, acc3)
    dummy = items

    slots = tiles * positions
    ids = jnp.concatenate([ids_ref[:, 128 * t : 128 * (t + 1)] for t in range(tiles)], axis=0)
    lengths = jnp.concatenate(
        [jnp.broadcast_to(len_ref[:, 128 * t : 128 * (t + 1)], (positions, 128)) for t in range(tiles)], axis=0
    )
    r = iota((slots, 128), 0)
    lane = iota((slots, 128), 1)
    local = ids - base
    live = (local >= 0) & (local < rows) & (lax.rem(r, positions) < lengths)
    item = lax.div(r, positions) * 128 + lane
    per = items // (NX * NZ)
    block = lax.div(item, per)
    dest = (lax.rem(block, NX) * NZ + lax.div(block, NX)) * per + lax.rem(item, per)
    code_ref[...] = local * 2048 + dest
    livef = jnp.where(live, f32(1.0), f32(0.0)).astype(bf16)
    below = jnp.where(iota((slots, slots), 0) >= iota((slots, slots), 1), f32(1.0), f32(0.0)).astype(bf16)
    order = jnp.dot(below, livef, preferred_element_type=f32)
    rank_ref[...] = jnp.where(live, order - 1.0, f32(-1.0)).astype(i32)
    counts = order[slots - 1 : slots, :].astype(i32)
    most = jnp.max(counts)

    for acc in accs:
        acc[...] = jnp.zeros_like(acc)

    def convert(c):
        loads[c].wait()

        @pl.loop(0, chunk // 256)
        def _(s):
            at = pl.ds(pl.multiple_of(c * chunk + s * 256, 256), 256)
            tab[at, :] = stage[at, :].astype(f32)

    def make_list(first):
        for k in range(DEPTH):
            found = jnp.sum(
                jnp.where(rank_ref[...] == first + k, code_ref[...], 0), axis=0, keepdims=True
            )
            list_ref[k : k + 1, :] = jnp.where(counts > first + k, found, dummy)
        list_ref[DEPTH : DEPTH + 1, :] = jnp.clip(counts - first, 0, DEPTH)

    def add_listed():
        @pl.loop(0, 128)
        def _(at):
            n = slist[DEPTH, at]

            def group(g, _):
                for q in range(PARTS):
                    code = slist[g * PARTS + q, at]
                    row = lax.shift_right_logical(code, 11)
                    to = code & 2047
                    accs[q][pl.ds(to, 1), :] += tab[pl.ds(row, 1), :]
                return 0

            lax.fori_loop(0, lax.shift_right_logical(n + PARTS - 1, 2), group, 0)

    make_list(0)
    copy = pltpu.make_async_copy(list_ref, slist, list_sem)
    copy.start()
    for c in range(CHUNKS):
        convert(c)
    copy.wait()
    add_listed()

    def more(b, _):
        make_list(b * DEPTH)
        copy = pltpu.make_async_copy(list_ref, slist, list_sem)
        copy.start()
        copy.wait()
        add_listed()
        return 0

    lax.fori_loop(1, lax.div(most + DEPTH - 1, DEPTH), more, 0)

    eye = iota((128, 128), 0) == iota((128, 128), 1)
    ones = jnp.ones((128, 128), bf16)
    for b in range(tiles):
        parts = []
        for h in range(128 // per):
            to = b * (128 // per) + h
            t = (to % NZ) * NX + to // NZ
            parts.append(len_ref[:, t * per : (t + 1) * per])
        row = jnp.concatenate(parts, axis=1).astype(f32)
        spread = jnp.where(eye, jnp.broadcast_to(row, (128, 128)), f32(0.0)).astype(bf16)
        column = jnp.dot(spread, ones, preferred_element_type=f32)
        at = pl.ds(128 * b, 128)
        out_ref[at, :] = (acc0[at, :] + acc1[at, :] + acc2[at, :] + acc3[at, :]) / column


def pool(ids_t, lengths, table):
    rows, width = table.shape
    positions, items = ids_t.shape
    slots = positions * items // 128
    vmem = pl.BlockSpec(memory_space=pltpu.VMEM)
    return pl.pallas_call(
        pool_kernel,
        name="pool",
        out_shape=jax.ShapeDtypeStruct((items, width), f32),
        in_specs=[vmem, vmem, pl.BlockSpec(memory_space=pltpu.HBM)],
        out_specs=vmem,
        scratch_shapes=[
            pltpu.VMEM((rows, width), bf16),
            pltpu.VMEM((rows, width), f32),
            *[pltpu.VMEM((items + 8, width), f32)] * PARTS,
            pltpu.VMEM((slots, 128), i32),
            pltpu.VMEM((slots, 128), i32),
            pltpu.VMEM((DEPTH + 8, 128), i32),
            pltpu.SMEM((DEPTH + 8, 128), i32),
            pltpu.SemaphoreType.DMA((CHUNKS,)),
            pltpu.SemaphoreType.DMA,
        ],
        cost_estimate=pl.CostEstimate(flops=10**8, bytes_accessed=9 * 2**20, transcendentals=0),
    )(ids_t, lengths, table)


def split_up(value, dim, size):
    lengths = value.shape
    parts = value.reshape(*lengths[:dim], size, lengths[dim] // size, *lengths[dim + 1 :])
    return jnp.moveaxis(parts, dim, 0)


def summed_on_arrival(value, axis, dim):
    size = lax.axis_size(axis)
    parts = lax.all_to_all(split_up(value, dim, size), axis, 0, 0, tiled=True)
    return jnp.sum(parts, axis=0)


def in_order(parts, dim):
    parts = jnp.moveaxis(parts, 0, dim)
    lengths = parts.shape
    return parts.reshape(*lengths[:dim], lengths[dim] * lengths[dim + 1], *lengths[dim + 2 :])


def copy_for_each(value, axis):
    copies = jnp.broadcast_to(value, (lax.axis_size(axis), *value.shape))
    return lax.all_to_all(copies, axis, split_axis=0, concat_axis=0, tiled=True)


def gather_directly(value, axis, dim):
    return in_order(copy_for_each(value, axis), dim)


def over_copies(value, axis):
    everything = copy_for_each(value, axis)
    return jnp.sum(everything, axis=0)


def in_one(arrays, axis):
    ends = [0]
    for a in arrays:
        ends.append(ends[-1] + a.size)
    total = over_copies(jnp.concatenate([a.ravel() for a in arrays]), axis)
    return tuple((total[b:e].reshape(a.shape) for a, b, e in zip(arrays, ends, ends[1:])))


def unit_rows(vectors):
    return vectors * lax.rsqrt(jnp.mean(vectors * vectors, axis=-1, keepdims=True) + epsilon)


def lookup_pool(bag_part, length_part, table, row_base):
    rows_total = table.shape[0]
    local = bag_part - row_base
    inside = (local >= 0) & (local < rows_total)
    valid = lax.broadcasted_iota(jnp.int32, bag_part.shape, 1) < length_part[:, None]
    keeping = inside & valid
    picked = jnp.take(table, jnp.clip(local, 0, rows_total - 1), axis=0).astype(jnp.float32)
    summed = jnp.sum(jnp.where(keeping[:, :, None], picked, jnp.float32(0.0)), axis=1)
    return summed / length_part[:, None].astype(jnp.float32)


def user_tower(features, user_w1, user_w2):
    user_hidden = jax.nn.gelu(
        jnp.dot(features, user_w1, preferred_element_type=jnp.float32), approximate=False
    ).astype(jnp.bfloat16)
    return unit_rows(jnp.dot(user_hidden, user_w2, preferred_element_type=jnp.float32))


def body(
    tables, bag_ids, bag_lengths, item_weight, user_features, user_w1, user_w2, positive_items
):
    table = tables[0]
    own_ids = bag_ids[0]
    own_lengths = bag_lengths[0]
    num_cand = lax.axis_size("cand")
    num_dp = lax.axis_size("dp")
    width = table.shape[1]
    embed = item_weight.shape[1]
    table_count = item_weight.shape[0] // width
    partial = pool(own_ids.T, own_lengths[None, :], table)
    per = partial.shape[0] // (NX * NZ)
    partial = partial.reshape(NX, NZ, per, width).transpose(1, 0, 2, 3).reshape(partial.shape)
    pooled = summed_on_arrival(partial, "tab", 0)
    groups = num_cand * num_dp
    shaped = pooled.reshape(1, groups, pooled.shape[0] // groups, width)
    weight_blocks = item_weight.astype(jnp.float32).reshape(table_count, width, embed)
    stacked = lax.all_to_all(shaped, ("cand", "dp"), split_axis=1, concat_axis=0, tiled=True)[:, 0]
    item_pre = jnp.einsum(
        "fbe,feh->bh",
        stacked,
        weight_blocks,
        precision=lax.Precision.HIGHEST,
        preferred_element_type=jnp.float32,
    )
    item_emb = unit_rows(item_pre)
    scale = logit_scale / embed
    per_block = item_emb.shape[0]
    cand_index = lax.axis_index("cand")

    def make_adder(user_emb, positives):

        def add_scores(carry, piece, global_id):
            scores = (
                lax.dot_general(
                    user_emb,
                    piece,
                    (((1,), (1,)), ((), ())),
                    precision=lax.Precision.HIGHEST,
                    preferred_element_type=jnp.float32,
                )
                * scale
            )
            sums = jnp.sum(jnp.exp(scores), axis=1)
            positive = jnp.sum(
                jnp.where(global_id == positives[:, None], scores, jnp.float32(0.0)), axis=1
            )
            return (sums, positive)

        return add_scores

    user_emb = user_tower(user_features, user_w1, user_w2)
    users_here = user_emb.shape[0]
    start_carry = (jnp.zeros((users_here,), jnp.float32), jnp.zeros((users_here,), jnp.float32))
    add_scores = make_adder(user_emb, positive_items)
    piece = gather_directly(item_emb, ("tab", "dp"), 0)
    place = lax.broadcasted_iota(jnp.int32, (1, piece.shape[0]), 1)
    group = place // per_block
    within = place % per_block
    global_id = (
        (group // num_dp * num_cand + cand_index) * num_dp + group % num_dp
    ) * per_block + within
    partial_sums = add_scores(start_carry, piece, global_id)
    sums, positive = in_one((partial_sums[0], partial_sums[1]), "cand")
    user_loss = jnp.log(sums) - positive
    return (item_emb, user_loss)


def solution(mesh):
    placed = (
        P(("cand", "dp"), "tab", None),
        P(("cand", "dp"), None, None),
        P(("cand", "dp"), None),
        P(),
        P(("tab", "dp"), None),
        P(),
        P(),
        P(("tab", "dp")),
    )
    return jax.shard_map(
        body,
        mesh=mesh,
        in_specs=placed,
        out_specs=(P(("tab", "cand", "dp"), None), P(("tab", "dp"))),
        check_vma=False,
    )
```

```python
import functools
import jax
import jax.numpy as jnp
from jax import lax
from jax.experimental import pallas as pl
from jax.experimental.pallas import tpu as pltpu
from jax.sharding import PartitionSpec as P

MESH = pl.DeviceIdType.MESH
f32, bf16, i32 = jnp.float32, jnp.bfloat16, jnp.int32
epsilon = 1e-06
logit_scale = 20.0
NX, NZ = 4, 4
PARTS = 4
DEPTH = 16
CHUNKS = 8


def iota(shape, dim):
    return lax.broadcasted_iota(i32, shape, dim)


def pool_kernel(ids_ref, len_ref, table_ref, out_ref, stage, tab, acc0, acc1, acc2, acc3,
                rank_ref, code_ref, list_ref, slist, load_sems, list_sem):
    rows = table_ref.shape[0]
    positions, items = ids_ref.shape
    tiles = items // 128
    chunk = rows // CHUNKS
    base = lax.axis_index("tab") * rows
    loads = [
        pltpu.make_async_copy(
            table_ref.at[pl.ds(c * chunk, chunk)], stage.at[pl.ds(c * chunk, chunk)], load_sems.at[c]
        )
        for c in range(CHUNKS)
    ]
    for load in loads:
        load.start()
    accs = (acc0, acc1, acc2, acc3)
    dummy = items

    slots = tiles * positions
    ids = jnp.concatenate([ids_ref[:, 128 * t : 128 * (t + 1)] for t in range(tiles)], axis=0)
    lengths = jnp.concatenate(
        [jnp.broadcast_to(len_ref[:, 128 * t : 128 * (t + 1)], (positions, 128)) for t in range(tiles)], axis=0
    )
    r = iota((slots, 128), 0)
    lane = iota((slots, 128), 1)
    local = ids - base
    live = (local >= 0) & (local < rows) & (lax.rem(r, positions) < lengths)
    item = lax.div(r, positions) * 128 + lane
    per = items // (NX * NZ)
    block = lax.div(item, per)
    dest = (lax.rem(block, NX) * NZ + lax.div(block, NX)) * per + lax.rem(item, per)
    code_ref[...] = local * 2048 + dest
    livef = jnp.where(live, f32(1.0), f32(0.0)).astype(bf16)
    below = jnp.where(iota((slots, slots), 0) >= iota((slots, slots), 1), f32(1.0), f32(0.0)).astype(bf16)
    order = jnp.dot(below, livef, preferred_element_type=f32)
    rank_ref[...] = jnp.where(live, order - 1.0, f32(-1.0)).astype(i32)
    counts = order[slots - 1 : slots, :].astype(i32)
    most = jnp.max(counts)

    for acc in accs:
        acc[...] = jnp.zeros_like(acc)

    def convert(c):
        loads[c].wait()

        @pl.loop(0, chunk // 256)
        def _(s):
            at = pl.ds(pl.multiple_of(c * chunk + s * 256, 256), 256)
            tab[at, :] = stage[at, :].astype(f32)

    def make_list(first):
        for k in range(DEPTH):
            found = jnp.sum(
                jnp.where(rank_ref[...] == first + k, code_ref[...], 0), axis=0, keepdims=True
            )
            list_ref[k : k + 1, :] = jnp.where(counts > first + k, found, dummy)
        list_ref[DEPTH : DEPTH + 1, :] = jnp.clip(counts - first, 0, DEPTH)

    def add_listed():
        @pl.loop(0, 128)
        def _(at):
            n = slist[DEPTH, at]

            def group(g, _):
                for q in range(PARTS):
                    code = slist[g * PARTS + q, at]
                    row = lax.shift_right_logical(code, 11)
                    to = code & 2047
                    accs[q][pl.ds(to, 1), :] += tab[pl.ds(row, 1), :]
                return 0

            lax.fori_loop(0, lax.shift_right_logical(n + PARTS - 1, 2), group, 0)

    make_list(0)
    copy = pltpu.make_async_copy(list_ref, slist, list_sem)
    copy.start()
    for c in range(CHUNKS):
        convert(c)
    copy.wait()
    add_listed()

    def more(b, _):
        make_list(b * DEPTH)
        copy = pltpu.make_async_copy(list_ref, slist, list_sem)
        copy.start()
        copy.wait()
        add_listed()
        return 0

    lax.fori_loop(1, lax.div(most + DEPTH - 1, DEPTH), more, 0)

    eye = iota((128, 128), 0) == iota((128, 128), 1)
    ones = jnp.ones((128, 128), bf16)
    for b in range(tiles):
        parts = []
        for h in range(128 // per):
            to = b * (128 // per) + h
            t = (to % NZ) * NX + to // NZ
            parts.append(len_ref[:, t * per : (t + 1) * per])
        row = jnp.concatenate(parts, axis=1).astype(f32)
        spread = jnp.where(eye, jnp.broadcast_to(row, (128, 128)), f32(0.0)).astype(bf16)
        column = jnp.dot(spread, ones, preferred_element_type=f32)
        at = pl.ds(128 * b, 128)
        out_ref[at, :] = (acc0[at, :] + acc1[at, :] + acc2[at, :] + acc3[at, :]) / column


def pool(ids_t, lengths, table):
    rows, width = table.shape
    positions, items = ids_t.shape
    slots = positions * items // 128
    vmem = pl.BlockSpec(memory_space=pltpu.VMEM)
    return pl.pallas_call(
        pool_kernel,
        name="pool",
        out_shape=jax.ShapeDtypeStruct((items, width), f32),
        in_specs=[vmem, vmem, pl.BlockSpec(memory_space=pltpu.HBM)],
        out_specs=vmem,
        scratch_shapes=[
            pltpu.VMEM((rows, width), bf16),
            pltpu.VMEM((rows, width), f32),
            *[pltpu.VMEM((items + 8, width), f32)] * PARTS,
            pltpu.VMEM((slots, 128), i32),
            pltpu.VMEM((slots, 128), i32),
            pltpu.VMEM((DEPTH + 8, 128), i32),
            pltpu.SMEM((DEPTH + 8, 128), i32),
            pltpu.SemaphoreType.DMA((CHUNKS,)),
            pltpu.SemaphoreType.DMA,
        ],
        cost_estimate=pl.CostEstimate(flops=10**8, bytes_accessed=9 * 2**20, transcendentals=0),
    )(ids_t, lengths, table)


def split2(v):
    high = v.astype(bf16)
    return high, (v - high.astype(f32)).astype(bf16)


def unit_rows(v):
    return v * lax.rsqrt(jnp.mean(v * v, axis=-1, keepdims=True) + epsilon)


PLAN = (1, 2, 1, 1, 3)
USERS_AT_ONCE = 256


def step_kernel(part_ref, weight_ref, x_ref, w1_ref, w2_ref, place_ref, item_ref, loss_ref,
                xv, w1v, w2v, wv, high_ref, low_ref, recvx, sendz, recvz, sendt, recvt, embed_ref,
                gathered, stats, others, load_sems, sx, rx, sz, rz, st, rt, sg, rg, ss, rs):
    tab, cand, dp = lax.axis_index("tab"), lax.axis_index("cand"), lax.axis_index("dp")
    xi, zi = lax.rem(tab, NX), lax.div(tab, NX)
    ntab, ncand, ndp = NX * NZ, 4, 4
    width = part_ref.shape[1]
    per = part_ref.shape[0] // ntab
    groups = ncand * ndp
    own = per // groups
    table = cand * ndp + dp

    def local(src, dst, k):
        copy = pltpu.make_async_copy(src, dst, load_sems.at[k])
        copy.start()
        return copy

    loads = [
        local(x_ref, xv, 0),
        local(w1_ref, w1v, 1),
        local(w2_ref, w2v, 2),
        local(weight_ref.at[pl.ds(pl.multiple_of(table * width, width), width)], wv, 3),
    ]

    barrier = pltpu.get_barrier_semaphore()

    @pl.loop(1, ntab * ndp)
    def _(k):
        peer = lax.rem(tab * ndp + dp + k, ntab * ndp)
        pl.semaphore_signal(
            barrier, inc=1, device_id=(lax.div(peer, ndp), cand, lax.rem(peer, ndp)), device_id_type=MESH
        )

    @pl.loop(ndp, groups)
    def _(k):
        peer = lax.rem(cand * ndp + k, groups)
        pl.semaphore_signal(
            barrier, inc=1, device_id=(tab, lax.div(peer, ndp), lax.rem(peer, ndp)), device_id_type=MESH
        )

    done = [0]

    def tower(chunks):
        if done[0] == 0:
            for k in range(3):
                loads[k].wait()
        first = done[0]
        done[0] += chunks

        @pl.loop(first, first + chunks)
        def _(c):
            at = pl.ds(pl.multiple_of(c * USERS_AT_ONCE, USERS_AT_ONCE), USERS_AT_ONCE)
            hidden = jnp.dot(xv[at, :], w1v[...], preferred_element_type=f32)
            hidden = (0.5 * hidden * (1.0 + lax.erf(hidden * f32(0.5**0.5)))).astype(bf16)
            users = unit_rows(jnp.dot(hidden, w2v[...], preferred_element_type=f32))
            high, low = split2(users * (logit_scale / users.shape[1]))
            high_ref[at, :] = high
            low_ref[at, :] = low

    tower(PLAN[0])
    pl.semaphore_wait(barrier, ntab * ndp - 1 + groups - ndp)

    xcopies = []
    turns = (2, 1, 3, 0)
    for n, k in enumerate(turns):
        zp = lax.rem(zi + k, NZ)
        row = []
        for o in range(1, NX):
            xp = lax.rem(xi + o, NX)
            src = part_ref.at[pl.ds(pl.multiple_of((xp * NZ + zp) * per, per), per)]
            copy = pltpu.make_async_remote_copy(
                src_ref=src,
                dst_ref=recvx.at[n, o - 1],
                send_sem=sx.at[n, o - 1],
                recv_sem=rx.at[n, o - 1],
                device_id=(zi * NX + xp, cand, dp),
                device_id_type=MESH,
            )
            copy.start()
            row.append(copy)
        xcopies.append(row)

    tower(PLAN[1])

    zcopies = []
    pooled = None
    for n, k in enumerate(turns):
        zp = lax.rem(zi + k, NZ)
        for copy in xcopies[n]:
            copy.wait_recv()
        mine = part_ref[pl.ds(pl.multiple_of((xi * NZ + zp) * per, per), per), :]
        total = mine + recvx[n, 0] + recvx[n, 1] + recvx[n, 2]
        if k == 0:
            pooled = total
        else:
            sendz[k - 1] = total
            copy = pltpu.make_async_remote_copy(
                src_ref=sendz.at[k - 1],
                dst_ref=recvz.at[k - 1],
                send_sem=sz.at[k - 1],
                recv_sem=rz.at[k - 1],
                device_id=(zp * NX + xi, cand, dp),
                device_id_type=MESH,
            )
            copy.start()
            zcopies.append(copy)
    tower(PLAN[2])
    loads[3].wait()
    for copy in zcopies:
        copy.wait_recv()
    pooled = pooled + recvz[0] + recvz[1] + recvz[2]

    p0 = pooled.astype(bf16)
    rest = pooled - p0.astype(f32)
    p1 = rest.astype(bf16)
    p2 = (rest - p1.astype(f32)).astype(bf16)
    terms = jnp.dot(jnp.concatenate([p0, p1, p2], axis=0), wv[...], preferred_element_type=f32)
    terms = terms[:per] + terms[per : 2 * per] + terms[2 * per :]
    for b in range(groups):
        sendt[b] = terms[b * own : (b + 1) * own, :]

    @pl.loop(1, groups)
    def _(k):
        peer = lax.rem(table + k, groups)
        pltpu.make_async_remote_copy(
            src_ref=sendt.at[peer],
            dst_ref=recvt.at[k - 1],
            send_sem=st,
            recv_sem=rt,
            device_id=(tab, lax.div(peer, ndp), lax.rem(peer, ndp)),
            device_id_type=MESH,
        ).start()

    tower(PLAN[3])
    all_t = pltpu.make_async_copy(recvt, recvt, rt)
    all_t.wait()
    total = sendt[table]
    for b in range(groups - 1):
        total = total + recvt[b]
    embed = unit_rows(total)
    embed_ref[...] = embed
    item_ref[...] = embed

    me = tab * ndp + dp

    @pl.loop(1, ntab * ndp)
    def _(k):
        peer = lax.rem(me + k, ntab * ndp)
        pltpu.make_async_remote_copy(
            src_ref=embed_ref,
            dst_ref=gathered.at[me],
            send_sem=sg,
            recv_sem=rg,
            device_id=(lax.div(peer, ndp), cand, lax.rem(peer, ndp)),
            device_id_type=MESH,
        ).start()

    gathered[me] = embed
    tower(PLAN[4])
    most = gathered.at[pl.ds(0, ntab * ndp - 1)]
    pltpu.make_async_copy(most, most, rg).wait()

    pieces = [gathered[b] for b in range(ntab * ndp)]
    items = jnp.concatenate(pieces, axis=0)
    item_high, item_low = split2(items)
    dims = (((1,), (1,)), ((), ()))
    count = items.shape[0]

    def score(c, _):
        at = pl.ds(pl.multiple_of(c * USERS_AT_ONCE, USERS_AT_ONCE), USERS_AT_ONCE)
        high = high_ref[at, :]
        scores = (
            lax.dot_general(item_high, high, dims, preferred_element_type=f32)
            + lax.dot_general(item_low, high, dims, preferred_element_type=f32)
            + lax.dot_general(item_high, low_ref[at, :], dims, preferred_element_type=f32)
        )
        sums = jnp.sum(jnp.exp(scores), axis=0, keepdims=True)
        for h in range(USERS_AT_ONCE // 128):
            line = c * (USERS_AT_ONCE // 128) + h
            place = place_ref[pl.ds(line, 1), :]
            block = lax.shift_right_logical(place, 4)
            here = lax.rem(block, ncand) == cand
            row = jnp.where(here, lax.div(block, ncand) * 16 + (place & 15), -1)
            part = scores[:, h * 128 : (h + 1) * 128]
            positive = jnp.sum(
                jnp.where(iota((count, 128), 0) == row, part, f32(0.0)), axis=0, keepdims=True
            )
            stats[pl.ds(line, 1), :] = sums[:, h * 128 : (h + 1) * 128]
            stats[pl.ds(line + place_ref.shape[0], 1), :] = positive
        return 0

    lax.fori_loop(0, xv.shape[0] // USERS_AT_ONCE, score, 0)

    scopies = []
    for o in range(1, ncand):
        copy = pltpu.make_async_remote_copy(
            src_ref=stats,
            dst_ref=others.at[o - 1],
            send_sem=ss.at[o - 1],
            recv_sem=rs.at[o - 1],
            device_id=(tab, lax.rem(cand + o, ncand), dp),
            device_id_type=MESH,
        )
        copy.start()
        scopies.append(copy)
    for row in xcopies:
        for copy in row:
            copy.wait_send()
    for copy in zcopies:
        copy.wait_send()
    pltpu.make_async_copy(recvt, recvt, st).wait()
    pltpu.make_async_copy(most, most, sg).wait()
    for copy in scopies:
        copy.wait_recv()
    both = stats[...] + others[0] + others[1] + others[2]
    lines = place_ref.shape[0]
    loss_ref[...] = jnp.log(both[:lines]) - both[lines:]
    for copy in scopies:
        copy.wait_send()


def step(partial, item_weight, features, user_w1, user_w2, places):
    items, width = partial.shape
    users, features_in = features.shape
    hidden, embed = user_w2.shape
    per = items // (NX * NZ)
    own = per // 16
    lines = users // 128
    vmem = pl.BlockSpec(memory_space=pltpu.VMEM)
    hbm = pl.BlockSpec(memory_space=pltpu.HBM)
    dma = pltpu.SemaphoreType.DMA
    return pl.pallas_call(
        step_kernel,
        name="step",
        out_shape=(jax.ShapeDtypeStruct((own, embed), f32), jax.ShapeDtypeStruct((lines, 128), f32)),
        in_specs=[vmem, hbm, hbm, hbm, hbm, vmem],
        out_specs=(vmem, vmem),
        scratch_shapes=[
            pltpu.VMEM((users, features_in), bf16),
            pltpu.VMEM((features_in, hidden), bf16),
            pltpu.VMEM((hidden, embed), bf16),
            pltpu.VMEM((width, embed), bf16),
            pltpu.VMEM((users, embed), bf16),
            pltpu.VMEM((users, embed), bf16),
            pltpu.VMEM((NZ, NX - 1, per, width), f32),
            pltpu.VMEM((NZ - 1, per, width), f32),
            pltpu.VMEM((NZ - 1, per, width), f32),
            pltpu.VMEM((16, own, embed), f32),
            pltpu.VMEM((15, own, embed), f32),
            pltpu.VMEM((own, embed), f32),
            pltpu.VMEM((64, own, embed), f32),
            pltpu.VMEM((2 * lines, 128), f32),
            pltpu.VMEM((3, 2 * lines, 128), f32),
            dma((4,)),
            dma((NZ, NX - 1)),
            dma((NZ, NX - 1)),
            dma((NZ - 1,)),
            dma((NZ - 1,)),
            dma,
            dma,
            dma,
            dma,
            dma((3,)),
            dma((3,)),
        ],
        compiler_params=pltpu.CompilerParams(collective_id=0, has_side_effects=True),
        cost_estimate=pl.CostEstimate(flops=5 * 10**9, bytes_accessed=5 * 2**20, transcendentals=0),
    )(partial, item_weight, features, user_w1, user_w2, places)


def body(
    tables, bag_ids, bag_lengths, item_weight, user_features, user_w1, user_w2, positive_items
):
    partial = pool(bag_ids[0].T, bag_lengths, tables[0])
    item_emb, loss = step(
        partial, item_weight, user_features, user_w1, user_w2, positive_items.reshape(-1, 128)
    )
    return (item_emb, loss.reshape(-1))


def solution(mesh):
    placed = (
        P(("cand", "dp"), "tab", None),
        P(("cand", "dp"), None, None),
        P(("cand", "dp"), None),
        P(),
        P(("tab", "dp"), None),
        P(),
        P(),
        P(("tab", "dp")),
    )
    return jax.shard_map(
        body,
        mesh=mesh,
        in_specs=placed,
        out_specs=(P(("tab", "cand", "dp"), None), P(("tab", "dp"))),
        check_vma=False,
    )
```

```python
import functools
import jax
import jax.numpy as jnp
from jax import lax
from jax.experimental import pallas as pl
from jax.experimental.pallas import tpu as pltpu
from jax.sharding import PartitionSpec as P

MESH = pl.DeviceIdType.MESH
f32, bf16, i32 = jnp.float32, jnp.bfloat16, jnp.int32
epsilon = 1e-06
logit_scale = 20.0
NX, NZ = 4, 4
PARTS = 4
DEPTH = 16
CHUNKS = 8
CAPACITY = 768


def iota(shape, dim):
    return lax.broadcasted_iota(i32, shape, dim)


def list_kernel(ids_ref, len_ref, table_ref, list_out, extra_ref, stage, tab, acc0, acc1, acc2, acc3,
                rank_ref, code_ref, list_ref, slist, load_sems, list_sem):
    rows = table_ref.shape[0]
    positions, items = ids_ref.shape
    tiles = items // 128
    chunk = rows // CHUNKS
    base = lax.axis_index("tab") * rows
    accs = (acc0, acc1, acc2, acc3)

    slots = tiles * positions
    ids = jnp.concatenate([ids_ref[:, 128 * t : 128 * (t + 1)] for t in range(tiles)], axis=0)
    lengths = jnp.concatenate(
        [jnp.broadcast_to(len_ref[:, 128 * t : 128 * (t + 1)], (positions, 128)) for t in range(tiles)], axis=0
    )
    r = iota((slots, 128), 0)
    lane = iota((slots, 128), 1)
    local = ids - base
    live = (local >= 0) & (local < rows) & (lax.rem(r, positions) < lengths)
    item = lax.div(r, positions) * 128 + lane
    per = items // (NX * NZ)
    block = lax.div(item, per)
    dest = (lax.rem(block, NX) * NZ + lax.div(block, NX)) * per + lax.rem(item, per)
    code = local * 2048 + dest + 1
    below = jnp.where(iota((slots, slots), 0) >= iota((slots, slots), 1), f32(1.0), f32(0.0)).astype(bf16)
    ones = jnp.ones((128, 128), bf16)

    def ordered(which):
        marks = jnp.where(which, f32(1.0), f32(0.0)).astype(bf16)
        order = jnp.dot(below, marks, preferred_element_type=f32)
        return order, jnp.where(which, order - 1.0, f32(-1.0)).astype(i32)

    order, rank = ordered(live)
    counts = jnp.minimum(order[slots - 1 : slots, :], f32(DEPTH))
    square = (128, 128)
    before = iota(square, 0) < iota(square, 1)
    offset = jnp.dot(
        jnp.broadcast_to(counts, (8, 128)).astype(bf16),
        jnp.where(before, f32(1.0), f32(0.0)).astype(bf16),
        preferred_element_type=f32,
    )
    spread = jnp.broadcast_to(counts, square)
    after = iota(square, 0) > iota(square, 1)
    eye = iota(square, 0) == iota(square, 1)
    column = jnp.dot(
        jnp.concatenate([jnp.where(after, spread, f32(0.0)), jnp.where(eye, spread, f32(0.0))], axis=0).astype(bf16),
        ones,
        preferred_element_type=f32,
    )
    offset_column, count_column = column[:128].astype(i32), column[128:].astype(i32)
    offset_row = offset[:1].astype(i32)
    lane_square = iota(square, 1)
    lines = iota((8, 128), 0)
    left, right = [], []
    for k in range(DEPTH):
        found = jnp.sum(jnp.where(rank == k, code, 0), axis=0, keepdims=True)
        where_to = jnp.broadcast_to(lax.shift_right_logical(offset_row + k, 7), (8, 128)) == lines
        left.append(
            jnp.concatenate(
                [
                    jnp.where(where_to, jnp.broadcast_to(lax.shift_right_logical(found, 7 * p) & 127, (8, 128)), 0)
                    for p in range(4)
                ],
                axis=0,
            ).astype(f32).astype(bf16)
        )
        hit = (((offset_column + k) & 127) == lane_square) & (count_column > k)
        right.append(jnp.where(hit, f32(1.0), f32(0.0)).astype(bf16))
    flat = jnp.dot(
        jnp.concatenate(left, axis=1), jnp.concatenate(right, axis=0), preferred_element_type=f32
    ).astype(i32)
    list_out[...] = flat[:8] + flat[8:16] * 128 + flat[16:24] * 16384 + flat[24:32] * 2097152
    extra_ref[...] = jnp.zeros_like(extra_ref)

    place = offset_row + rank
    over = live & ((rank >= DEPTH) | (place >= CAPACITY))
    beyond = jnp.max(jnp.where(over, f32(1.0), f32(0.0)))

    @pl.when(beyond > 0.0)
    def _():
        loads = [
            pltpu.make_async_copy(
                table_ref.at[pl.ds(c * chunk, chunk)], stage.at[pl.ds(c * chunk, chunk)], load_sems.at[c]
            )
            for c in range(CHUNKS)
        ]
        for load in loads:
            load.start()
        order, rank = ordered(over)
        rank_ref[...] = rank
        code_ref[...] = code
        counts = order[slots - 1 : slots, :].astype(i32)
        most = jnp.max(counts)
        for acc in accs:
            acc[...] = jnp.zeros_like(acc)
        for load in loads:
            load.wait()

        @pl.loop(0, rows // 256)
        def _(s):
            at = pl.ds(pl.multiple_of(s * 256, 256), 256)
            tab[at, :] = stage[at, :].astype(f32)

        def more(b, _):
            for k in range(DEPTH):
                found = jnp.sum(
                    jnp.where(rank_ref[...] == b * DEPTH + k, code_ref[...], 0), axis=0, keepdims=True
                )
                list_ref[k : k + 1, :] = found
            list_ref[DEPTH : DEPTH + 1, :] = jnp.clip(counts - b * DEPTH, 0, DEPTH)
            copy = pltpu.make_async_copy(list_ref, slist, list_sem)
            copy.start()
            copy.wait()

            @pl.loop(0, 128)
            def _(at):
                def group(g, _):
                    for q in range(PARTS):
                        code = slist[g * PARTS + q, at]
                        row = lax.shift_right_logical(code, 11)
                        to = code & 2047
                        accs[q][pl.ds(to, 1), :] += tab[pl.ds(row, 1), :]
                    return 0

                lax.fori_loop(0, lax.shift_right_logical(slist[DEPTH, at] + PARTS - 1, 2), group, 0)

            return 0

        lax.fori_loop(0, lax.div(most + DEPTH - 1, DEPTH), more, 0)
        extra_ref[...] = acc0[1 : items + 1, :] + acc1[1 : items + 1, :] + acc2[1 : items + 1, :] + acc3[1 : items + 1, :]


def make_list(ids_t, lengths, table):
    rows, width = table.shape
    positions, items = ids_t.shape
    slots = positions * items // 128
    vmem = pl.BlockSpec(memory_space=pltpu.VMEM)
    return pl.pallas_call(
        list_kernel,
        name="list",
        out_shape=(jax.ShapeDtypeStruct((8, 128), i32), jax.ShapeDtypeStruct((items, width), f32)),
        in_specs=[vmem, vmem, pl.BlockSpec(memory_space=pltpu.HBM)],
        out_specs=(vmem, vmem),
        scratch_shapes=[
            pltpu.VMEM((rows, width), bf16),
            pltpu.VMEM((rows, width), f32),
            *[pltpu.VMEM((items + 8, width), f32)] * PARTS,
            pltpu.VMEM((slots, 128), i32),
            pltpu.VMEM((slots, 128), i32),
            pltpu.VMEM((DEPTH + 8, 128), i32),
            pltpu.SMEM((DEPTH + 8, 128), i32),
            pltpu.SemaphoreType.DMA((CHUNKS,)),
            pltpu.SemaphoreType.DMA,
        ],
        compiler_params=pltpu.CompilerParams(vmem_limit_bytes=58 * 2**20),
        cost_estimate=pl.CostEstimate(flops=10**8, bytes_accessed=2**20, transcendentals=0),
    )(ids_t, lengths, table)


def split2(v):
    high = v.astype(bf16)
    return high, (v - high.astype(f32)).astype(bf16)


def unit_rows(v):
    return v * lax.rsqrt(jnp.mean(v * v, axis=-1, keepdims=True) + epsilon)


PLAN = (0, 3, 1, 1, 3)
USERS_AT_ONCE = 256
TOGETHER = 16


def step_kernel(slist, vlist, extra_ref, len_ref, table_ref, weight_ref, x_ref, w1_ref, w2_ref, place_ref, item_ref, loss_ref,
                stage, wide, listed, part_ref, xv, w1v, w2v, wv, high_ref, low_ref, recvx, sendz, recvz, sendt, recvt, embed_ref,
                gathered, stats, others, table_sems, load_sems, sx, rx, sz, rz, st, rt, sg, rg, ss, rs):
    tab, cand, dp = lax.axis_index("tab"), lax.axis_index("cand"), lax.axis_index("dp")
    xi, zi = lax.rem(tab, NX), lax.div(tab, NX)
    ntab, ncand, ndp = NX * NZ, 4, 4
    width = part_ref.shape[1]
    per = part_ref.shape[0] // ntab
    groups = ncand * ndp
    own = per // groups
    table = cand * ndp + dp

    def local(src, dst, k):
        copy = pltpu.make_async_copy(src, dst, load_sems.at[k])
        copy.start()
        return copy

    rows = table_ref.shape[0]
    chunk = rows // CHUNKS
    table_loads = []
    for c in range(CHUNKS):
        at = pl.ds(c * chunk, chunk)
        table_loads.append(pltpu.make_async_copy(table_ref.at[at], stage.at[at], table_sems.at[c]))
        table_loads[-1].start()

    loads = [
        local(x_ref, xv, 0),
        local(w1_ref, w1v, 1),
        local(w2_ref, w2v, 2),
        local(weight_ref.at[pl.ds(pl.multiple_of(table * width, width), width)], wv, 3),
    ]

    barrier = pltpu.get_barrier_semaphore()

    @pl.loop(1, ntab * ndp)
    def _(k):
        peer = lax.rem(tab * ndp + dp + k, ntab * ndp)
        pl.semaphore_signal(
            barrier, inc=1, device_id=(lax.div(peer, ndp), cand, lax.rem(peer, ndp)), device_id_type=MESH
        )

    @pl.loop(ndp, groups)
    def _(k):
        peer = lax.rem(cand * ndp + k, groups)
        pl.semaphore_signal(
            barrier, inc=1, device_id=(tab, lax.div(peer, ndp), lax.rem(peer, ndp)), device_id_type=MESH
        )

    done = [0]

    def tower(chunks):
        if done[0] == 0:
            for k in range(3):
                loads[k].wait()
        first = done[0]
        done[0] += chunks

        @pl.loop(first, first + chunks)
        def _(c):
            at = pl.ds(pl.multiple_of(c * USERS_AT_ONCE, USERS_AT_ONCE), USERS_AT_ONCE)
            hidden = jnp.dot(xv[at, :], w1v[...], preferred_element_type=f32)
            hidden = (0.5 * hidden * (1.0 + lax.erf(hidden * f32(0.5**0.5)))).astype(bf16)
            users = unit_rows(jnp.dot(hidden, w2v[...], preferred_element_type=f32))
            high, low = split2(users * (logit_scale / users.shape[1]))
            high_ref[at, :] = high
            low_ref[at, :] = low

    for c in range(CHUNKS):
        table_loads[c].wait()

        @pl.loop(0, chunk // 256)
        def _(s):
            at = pl.ds(pl.multiple_of(c * chunk + s * 256, 256), 256)
            wide[at, :] = stage[at, :].astype(f32)

    for line in range(CAPACITY // 128):

        @pl.loop(0, 128 // TOGETHER)
        def _(g):
            at = pl.multiple_of(g * TOGETHER, TOGETHER)
            fetched = []
            for q in range(TOGETHER):
                row = lax.shift_right_logical(slist[line, at + q], 11)
                fetched.append(wide[pl.ds(row, 1), :])
            for q in range(TOGETHER):
                listed[pl.ds(line * 128 + at + q, 1), :] = fetched[q]

    square = (128, 128)
    eye = iota(square, 0) == iota(square, 1)
    ones = jnp.ones(square, bf16)
    picked = listed[...].astype(bf16)
    wanted = vlist[...] & 2047
    for b in range(part_ref.shape[0] // 128):
        select = jnp.concatenate(
            [
                jnp.where(wanted[n : n + 1, :] == iota(square, 0) + (128 * b + 1), f32(1.0), f32(0.0)).astype(bf16)
                for n in range(CAPACITY // 128)
            ],
            axis=1,
        )
        ends = []
        for h in range(128 // per):
            to = b * (128 // per) + h
            t = (to % NZ) * NX + to // NZ
            ends.append(len_ref[:, t * per : (t + 1) * per])
        spread = jnp.broadcast_to(jnp.concatenate(ends, axis=1).astype(f32), square)
        column = jnp.dot(jnp.where(eye, spread, f32(0.0)).astype(bf16), ones, preferred_element_type=f32)
        at = pl.ds(128 * b, 128)
        part_ref[at, :] = (jnp.dot(select, picked, preferred_element_type=f32) + extra_ref[at, :]) / column

    if PLAN[0]:
        tower(PLAN[0])
    pl.semaphore_wait(barrier, ntab * ndp - 1 + groups - ndp)

    xcopies = []
    turns = (2, 1, 3, 0)
    for n, k in enumerate(turns):
        zp = lax.rem(zi + k, NZ)
        row = []
        for o in range(1, NX):
            xp = lax.rem(xi + o, NX)
            src = part_ref.at[pl.ds(pl.multiple_of((xp * NZ + zp) * per, per), per)]
            copy = pltpu.make_async_remote_copy(
                src_ref=src,
                dst_ref=recvx.at[n, o - 1],
                send_sem=sx.at[n, o - 1],
                recv_sem=rx.at[n, o - 1],
                device_id=(zi * NX + xp, cand, dp),
                device_id_type=MESH,
            )
            copy.start()
            row.append(copy)
        xcopies.append(row)

    tower(PLAN[1])

    zcopies = []
    pooled = None
    for n, k in enumerate(turns):
        zp = lax.rem(zi + k, NZ)
        for copy in xcopies[n]:
            copy.wait_recv()
        mine = part_ref[pl.ds(pl.multiple_of((xi * NZ + zp) * per, per), per), :]
        total = mine + recvx[n, 0] + recvx[n, 1] + recvx[n, 2]
        if k == 0:
            pooled = total
        else:
            sendz[k - 1] = total
            copy = pltpu.make_async_remote_copy(
                src_ref=sendz.at[k - 1],
                dst_ref=recvz.at[k - 1],
                send_sem=sz.at[k - 1],
                recv_sem=rz.at[k - 1],
                device_id=(zp * NX + xi, cand, dp),
                device_id_type=MESH,
            )
            copy.start()
            zcopies.append(copy)
    tower(PLAN[2])
    loads[3].wait()
    for copy in zcopies:
        copy.wait_recv()
    pooled = pooled + recvz[0] + recvz[1] + recvz[2]

    p0 = pooled.astype(bf16)
    rest = pooled - p0.astype(f32)
    p1 = rest.astype(bf16)
    p2 = (rest - p1.astype(f32)).astype(bf16)
    terms = jnp.dot(jnp.concatenate([p0, p1, p2], axis=0), wv[...], preferred_element_type=f32)
    terms = terms[:per] + terms[per : 2 * per] + terms[2 * per :]
    for b in range(groups):
        sendt[b] = terms[b * own : (b + 1) * own, :]

    @pl.loop(1, groups)
    def _(k):
        peer = lax.rem(table + k, groups)
        pltpu.make_async_remote_copy(
            src_ref=sendt.at[peer],
            dst_ref=recvt.at[k - 1],
            send_sem=st,
            recv_sem=rt,
            device_id=(tab, lax.div(peer, ndp), lax.rem(peer, ndp)),
            device_id_type=MESH,
        ).start()

    tower(PLAN[3])
    all_t = pltpu.make_async_copy(recvt, recvt, rt)
    all_t.wait()
    total = sendt[table]
    for b in range(groups - 1):
        total = total + recvt[b]
    embed = unit_rows(total)
    embed_ref[...] = embed
    item_ref[...] = embed

    me = tab * ndp + dp

    for k in turns:

        @pl.loop(0 if k else 1, NX * ndp)
        def _(n):
            zp = lax.rem(zi + k, NZ)
            xp = lax.rem(xi + lax.div(n, ndp), NX)
            pltpu.make_async_remote_copy(
                src_ref=embed_ref,
                dst_ref=gathered.at[me],
                send_sem=sg,
                recv_sem=rg,
                device_id=(zp * NX + xp, cand, lax.rem(dp + n, ndp)),
                device_id_type=MESH,
            ).start()

    gathered[me] = embed
    tower(PLAN[4])
    most = gathered.at[pl.ds(0, ntab * ndp - 1)]
    pltpu.make_async_copy(most, most, rg).wait()

    pieces = [gathered[b] for b in range(ntab * ndp)]
    items = jnp.concatenate(pieces, axis=0)
    item_high, item_low = split2(items)
    dims = (((1,), (1,)), ((), ()))
    count = items.shape[0]

    def score(c, _):
        at = pl.ds(pl.multiple_of(c * USERS_AT_ONCE, USERS_AT_ONCE), USERS_AT_ONCE)
        high = high_ref[at, :]
        scores = (
            lax.dot_general(item_high, high, dims, preferred_element_type=f32)
            + lax.dot_general(item_low, high, dims, preferred_element_type=f32)
            + lax.dot_general(item_high, low_ref[at, :], dims, preferred_element_type=f32)
        )
        sums = jnp.sum(jnp.exp(scores), axis=0, keepdims=True)
        for h in range(USERS_AT_ONCE // 128):
            line = c * (USERS_AT_ONCE // 128) + h
            place = place_ref[pl.ds(line, 1), :]
            block = lax.shift_right_logical(place, 4)
            here = lax.rem(block, ncand) == cand
            row = jnp.where(here, lax.div(block, ncand) * 16 + (place & 15), -1)
            part = scores[:, h * 128 : (h + 1) * 128]
            positive = jnp.sum(
                jnp.where(iota((count, 128), 0) == row, part, f32(0.0)), axis=0, keepdims=True
            )
            stats[pl.ds(line, 1), :] = sums[:, h * 128 : (h + 1) * 128]
            stats[pl.ds(line + place_ref.shape[0], 1), :] = positive
        return 0

    lax.fori_loop(0, xv.shape[0] // USERS_AT_ONCE, score, 0, unroll=4)

    scopies = []
    for o in range(1, ncand):
        copy = pltpu.make_async_remote_copy(
            src_ref=stats,
            dst_ref=others.at[o - 1],
            send_sem=ss.at[o - 1],
            recv_sem=rs.at[o - 1],
            device_id=(tab, lax.rem(cand + o, ncand), dp),
            device_id_type=MESH,
        )
        copy.start()
        scopies.append(copy)
    for row in xcopies:
        for copy in row:
            copy.wait_send()
    for copy in zcopies:
        copy.wait_send()
    pltpu.make_async_copy(recvt, recvt, st).wait()
    pltpu.make_async_copy(most, most, sg).wait()
    for copy in scopies:
        copy.wait_recv()
    both = stats[...] + others[0] + others[1] + others[2]
    lines = place_ref.shape[0]
    loss_ref[...] = jnp.log(both[:lines]) - both[lines:]
    for copy in scopies:
        copy.wait_send()


def step(flat, extra, lengths, table, item_weight, features, user_w1, user_w2, places):
    items, width = extra.shape
    rows = table.shape[0]
    users, features_in = features.shape
    hidden, embed = user_w2.shape
    per = items // (NX * NZ)
    own = per // 16
    lines = users // 128
    vmem = pl.BlockSpec(memory_space=pltpu.VMEM)
    hbm = pl.BlockSpec(memory_space=pltpu.HBM)
    dma = pltpu.SemaphoreType.DMA
    return pl.pallas_call(
        step_kernel,
        name="step",
        out_shape=(jax.ShapeDtypeStruct((own, embed), f32), jax.ShapeDtypeStruct((lines, 128), f32)),
        in_specs=[pl.BlockSpec(memory_space=pltpu.SMEM), vmem, vmem, vmem, hbm, hbm, hbm, hbm, hbm, vmem],
        out_specs=(vmem, vmem),
        scratch_shapes=[
            pltpu.VMEM((rows, width), bf16),
            pltpu.VMEM((rows, width), f32),
            pltpu.VMEM((CAPACITY, width), f32),
            pltpu.VMEM((items, width), f32),
            pltpu.VMEM((users, features_in), bf16),
            pltpu.VMEM((features_in, hidden), bf16),
            pltpu.VMEM((hidden, embed), bf16),
            pltpu.VMEM((width, embed), bf16),
            pltpu.VMEM((users, embed), bf16),
            pltpu.VMEM((users, embed), bf16),
            pltpu.VMEM((NZ, NX - 1, per, width), f32),
            pltpu.VMEM((NZ - 1, per, width), f32),
            pltpu.VMEM((NZ - 1, per, width), f32),
            pltpu.VMEM((16, own, embed), f32),
            pltpu.VMEM((15, own, embed), f32),
            pltpu.VMEM((own, embed), f32),
            pltpu.VMEM((64, own, embed), f32),
            pltpu.VMEM((2 * lines, 128), f32),
            pltpu.VMEM((3, 2 * lines, 128), f32),
            dma((CHUNKS,)),
            dma((4,)),
            dma((NZ, NX - 1)),
            dma((NZ, NX - 1)),
            dma((NZ - 1,)),
            dma((NZ - 1,)),
            dma,
            dma,
            dma,
            dma,
            dma((3,)),
            dma((3,)),
        ],
        compiler_params=pltpu.CompilerParams(
            collective_id=0, has_side_effects=True, vmem_limit_bytes=48 * 2**20
        ),
        cost_estimate=pl.CostEstimate(flops=5 * 10**9, bytes_accessed=5 * 2**20, transcendentals=0),
    )(flat, flat, extra, lengths, table, item_weight, features, user_w1, user_w2, places)


def body(
    tables, bag_ids, bag_lengths, item_weight, user_features, user_w1, user_w2, positive_items
):
    flat, extra = make_list(bag_ids[0].T, bag_lengths, tables[0])
    item_emb, loss = step(
        flat, extra, bag_lengths, tables[0], item_weight, user_features, user_w1, user_w2, positive_items.reshape(-1, 128)
    )
    return (item_emb, loss.reshape(-1))


def solution(mesh):
    placed = (
        P(("cand", "dp"), "tab", None),
        P(("cand", "dp"), None, None),
        P(("cand", "dp"), None),
        P(),
        P(("tab", "dp"), None),
        P(),
        P(),
        P(("tab", "dp")),
    )
    return jax.shard_map(
        body,
        mesh=mesh,
        in_specs=placed,
        out_specs=(P(("tab", "cand", "dp"), None), P(("tab", "dp"))),
        check_vma=False,
    )
```

```python
import functools
import jax
import jax.numpy as jnp
from jax import lax
from jax.experimental import pallas as pl
from jax.experimental.pallas import tpu as pltpu
from jax.sharding import PartitionSpec as P

MESH = pl.DeviceIdType.MESH
f32, bf16, i32 = jnp.float32, jnp.bfloat16, jnp.int32
epsilon = 1e-06
logit_scale = 20.0
NX, NZ = 4, 4
PARTS = 4
DEPTH = 16
CHUNKS = 8
CAPACITY = 768


def iota(shape, dim):
    return lax.broadcasted_iota(i32, shape, dim)


def list_kernel(ids_ref, len_ref, table_ref, list_out, extra_ref, stage, tab, acc0, acc1, acc2, acc3,
                rank_ref, code_ref, list_ref, slist, load_sems, list_sem):
    rows = table_ref.shape[0]
    positions, items = ids_ref.shape
    tiles = items // 128
    chunk = rows // CHUNKS
    base = lax.axis_index("tab") * rows
    accs = (acc0, acc1, acc2, acc3)

    slots = tiles * positions
    ids = jnp.concatenate([ids_ref[:, 128 * t : 128 * (t + 1)] for t in range(tiles)], axis=0)
    lengths = jnp.concatenate(
        [jnp.broadcast_to(len_ref[:, 128 * t : 128 * (t + 1)], (positions, 128)) for t in range(tiles)], axis=0
    )
    r = iota((slots, 128), 0)
    lane = iota((slots, 128), 1)
    local = ids - base
    live = (local >= 0) & (local < rows) & (lax.rem(r, positions) < lengths)
    item = lax.div(r, positions) * 128 + lane
    per = items // (NX * NZ)
    block = lax.div(item, per)
    dest = (lax.rem(block, NX) * NZ + lax.div(block, NX)) * per + lax.rem(item, per)
    code = local * 2048 + dest + 1
    below = jnp.where(iota((slots, slots), 0) >= iota((slots, slots), 1), f32(1.0), f32(0.0)).astype(bf16)
    ones = jnp.ones((128, 128), bf16)

    def ordered(which):
        marks = jnp.where(which, f32(1.0), f32(0.0)).astype(bf16)
        order = jnp.dot(below, marks, preferred_element_type=f32)
        return order, jnp.where(which, order - 1.0, f32(-1.0)).astype(i32)

    order, rank = ordered(live)
    counts = jnp.minimum(order[slots - 1 : slots, :], f32(DEPTH))
    square = (128, 128)
    before = iota(square, 0) < iota(square, 1)
    offset = jnp.dot(
        jnp.broadcast_to(counts, (8, 128)).astype(bf16),
        jnp.where(before, f32(1.0), f32(0.0)).astype(bf16),
        preferred_element_type=f32,
    )
    spread = jnp.broadcast_to(counts, square)
    after = iota(square, 0) > iota(square, 1)
    eye = iota(square, 0) == iota(square, 1)
    column = jnp.dot(
        jnp.concatenate([jnp.where(after, spread, f32(0.0)), jnp.where(eye, spread, f32(0.0))], axis=0).astype(bf16),
        ones,
        preferred_element_type=f32,
    )
    offset_column, count_column = column[:128].astype(i32), column[128:].astype(i32)
    offset_row = offset[:1].astype(i32)
    lane_square = iota(square, 1)
    lines = iota((8, 128), 0)
    left, right = [], []
    for k in range(DEPTH):
        found = jnp.sum(jnp.where(rank == k, code, 0), axis=0, keepdims=True)
        where_to = jnp.broadcast_to(lax.shift_right_logical(offset_row + k, 7), (8, 128)) == lines
        left.append(
            jnp.concatenate(
                [
                    jnp.where(where_to, jnp.broadcast_to(lax.shift_right_logical(found, 7 * p) & 127, (8, 128)), 0)
                    for p in range(4)
                ],
                axis=0,
            ).astype(f32).astype(bf16)
        )
        hit = (((offset_column + k) & 127) == lane_square) & (count_column > k)
        right.append(jnp.where(hit, f32(1.0), f32(0.0)).astype(bf16))
    flat = jnp.dot(
        jnp.concatenate(left, axis=1), jnp.concatenate(right, axis=0), preferred_element_type=f32
    ).astype(i32)
    list_out[...] = flat[:8] + flat[8:16] * 128 + flat[16:24] * 16384 + flat[24:32] * 2097152
    extra_ref[...] = jnp.zeros_like(extra_ref)

    place = offset_row + rank
    over = live & ((rank >= DEPTH) | (place >= CAPACITY))
    beyond = jnp.max(jnp.where(over, f32(1.0), f32(0.0)))

    @pl.when(beyond > 0.0)
    def _():
        loads = [
            pltpu.make_async_copy(
                table_ref.at[pl.ds(c * chunk, chunk)], stage.at[pl.ds(c * chunk, chunk)], load_sems.at[c]
            )
            for c in range(CHUNKS)
        ]
        for load in loads:
            load.start()
        order, rank = ordered(over)
        rank_ref[...] = rank
        code_ref[...] = code
        counts = order[slots - 1 : slots, :].astype(i32)
        most = jnp.max(counts)
        for acc in accs:
            acc[...] = jnp.zeros_like(acc)
        for load in loads:
            load.wait()

        @pl.loop(0, rows // 256)
        def _(s):
            at = pl.ds(pl.multiple_of(s * 256, 256), 256)
            tab[at, :] = stage[at, :].astype(f32)

        def more(b, _):
            for k in range(DEPTH):
                found = jnp.sum(
                    jnp.where(rank_ref[...] == b * DEPTH + k, code_ref[...], 0), axis=0, keepdims=True
                )
                list_ref[k : k + 1, :] = found
            list_ref[DEPTH : DEPTH + 1, :] = jnp.clip(counts - b * DEPTH, 0, DEPTH)
            copy = pltpu.make_async_copy(list_ref, slist, list_sem)
            copy.start()
            copy.wait()

            @pl.loop(0, 128)
            def _(at):
                def group(g, _):
                    for q in range(PARTS):
                        code = slist[g * PARTS + q, at]
                        row = lax.shift_right_logical(code, 11)
                        to = code & 2047
                        accs[q][pl.ds(to, 1), :] += tab[pl.ds(row, 1), :]
                    return 0

                lax.fori_loop(0, lax.shift_right_logical(slist[DEPTH, at] + PARTS - 1, 2), group, 0)

            return 0

        lax.fori_loop(0, lax.div(most + DEPTH - 1, DEPTH), more, 0)
        extra_ref[...] = acc0[1 : items + 1, :] + acc1[1 : items + 1, :] + acc2[1 : items + 1, :] + acc3[1 : items + 1, :]


def make_list(ids_t, lengths, table):
    rows, width = table.shape
    positions, items = ids_t.shape
    slots = positions * items // 128
    vmem = pl.BlockSpec(memory_space=pltpu.VMEM)
    return pl.pallas_call(
        list_kernel,
        name="list",
        out_shape=(jax.ShapeDtypeStruct((8, 128), i32), jax.ShapeDtypeStruct((items, width), f32)),
        in_specs=[vmem, vmem, pl.BlockSpec(memory_space=pltpu.HBM)],
        out_specs=(vmem, vmem),
        scratch_shapes=[
            pltpu.VMEM((rows, width), bf16),
            pltpu.VMEM((rows, width), f32),
            *[pltpu.VMEM((items + 8, width), f32)] * PARTS,
            pltpu.VMEM((slots, 128), i32),
            pltpu.VMEM((slots, 128), i32),
            pltpu.VMEM((DEPTH + 8, 128), i32),
            pltpu.SMEM((DEPTH + 8, 128), i32),
            pltpu.SemaphoreType.DMA((CHUNKS,)),
            pltpu.SemaphoreType.DMA,
        ],
        compiler_params=pltpu.CompilerParams(vmem_limit_bytes=52 * 2**20),
        cost_estimate=pl.CostEstimate(flops=10**8, bytes_accessed=2**20, transcendentals=0),
    )(ids_t, lengths, table)


def split2(v):
    high = v.astype(bf16)
    return high, (v - high.astype(f32)).astype(bf16)


def unit_rows(v):
    return v * lax.rsqrt(jnp.mean(v * v, axis=-1, keepdims=True) + epsilon)


PLAN = (0, 3, 1, 1, 3)
USERS_AT_ONCE = 256
TOGETHER = 16


def step_kernel(slist, vlist, extra_ref, len_ref, table_ref, weight_ref, xv, w1v, w2v, place_ref, item_ref, loss_ref,
                stage, wide, listed, part_ref, high_ref, low_ref, recvx, sendz, recvz, sendt, recvt, embed_ref,
                gathered, stats, others, table_sems, sx, rx, sz, rz, st, rt, sg, rg, ss, rs):
    tab, cand, dp = lax.axis_index("tab"), lax.axis_index("cand"), lax.axis_index("dp")
    xi, zi = lax.rem(tab, NX), lax.div(tab, NX)
    ntab, ncand, ndp = NX * NZ, 4, 4
    width = part_ref.shape[1]
    per = part_ref.shape[0] // ntab
    groups = ncand * ndp
    own = per // groups
    table = cand * ndp + dp

    rows = table_ref.shape[0]
    chunk = rows // CHUNKS
    table_loads = []
    for c in range(CHUNKS):
        at = pl.ds(c * chunk, chunk)
        table_loads.append(pltpu.make_async_copy(table_ref.at[at], stage.at[at], table_sems.at[c]))
        table_loads[-1].start()

    barrier = pltpu.get_barrier_semaphore()

    def greet(device):
        pl.semaphore_signal(barrier, inc=1, device_id=device, device_id_type=MESH)

    for a in (2, 3, 1, 0):
        for k in (2, 1, 3, 0):
            if a or k:
                greet((tab, lax.rem(cand + a, ncand), lax.rem(dp + k, ndp)))
    for k in range(1, NZ):
        greet((lax.rem(zi + k, NZ) * NX + xi, cand, dp))
    for k in range(1, NX):
        greet((zi * NX + lax.rem(xi + k, NX), cand, dp))

    done = [0]

    def tower(chunks):
        first = done[0]
        done[0] += chunks

        @pl.loop(first, first + chunks)
        def _(c):
            at = pl.ds(pl.multiple_of(c * USERS_AT_ONCE, USERS_AT_ONCE), USERS_AT_ONCE)
            hidden = jnp.dot(xv[at, :], w1v[...], preferred_element_type=f32)
            hidden = (0.5 * hidden * (1.0 + lax.erf(hidden * f32(0.5**0.5)))).astype(bf16)
            users = unit_rows(jnp.dot(hidden, w2v[...], preferred_element_type=f32))
            high, low = split2(users * (logit_scale / users.shape[1]))
            high_ref[at, :] = high
            low_ref[at, :] = low

    for c in range(CHUNKS):
        table_loads[c].wait()

        @pl.loop(0, chunk // 256)
        def _(s):
            at = pl.ds(pl.multiple_of(c * chunk + s * 256, 256), 256)
            wide[at, :] = stage[at, :].astype(f32)

    for line in range(CAPACITY // 128):

        @pl.loop(0, 128 // TOGETHER)
        def _(g):
            at = pl.multiple_of(g * TOGETHER, TOGETHER)
            fetched = []
            for q in range(TOGETHER):
                row = lax.shift_right_logical(slist[line, at + q], 11)
                fetched.append(wide[pl.ds(row, 1), :])
            for q in range(TOGETHER):
                listed[pl.ds(line * 128 + at + q, 1), :] = fetched[q]

    square = (128, 128)
    eye = iota(square, 0) == iota(square, 1)
    ones = jnp.ones(square, bf16)
    picked = listed[...].astype(bf16)
    wanted = vlist[...] & 2047
    for b in range(part_ref.shape[0] // 128):
        select = jnp.concatenate(
            [
                jnp.where(wanted[n : n + 1, :] == iota(square, 0) + (128 * b + 1), f32(1.0), f32(0.0)).astype(bf16)
                for n in range(CAPACITY // 128)
            ],
            axis=1,
        )
        ends = []
        for h in range(128 // per):
            to = b * (128 // per) + h
            t = (to % NZ) * NX + to // NZ
            ends.append(len_ref[:, t * per : (t + 1) * per])
        spread = jnp.broadcast_to(jnp.concatenate(ends, axis=1).astype(f32), square)
        column = jnp.dot(jnp.where(eye, spread, f32(0.0)).astype(bf16), ones, preferred_element_type=f32)
        at = pl.ds(128 * b, 128)
        part_ref[at, :] = (jnp.dot(select, picked, preferred_element_type=f32) + extra_ref[at, :]) / column

    if PLAN[0]:
        tower(PLAN[0])
    pl.semaphore_wait(barrier, groups - 1 + NZ - 1 + NX - 1)

    xcopies = []
    turns = (2, 1, 3, 0)
    for n, k in enumerate(turns):
        zp = lax.rem(zi + k, NZ)
        row = []
        for o in range(1, NX):
            xp = lax.rem(xi + o, NX)
            src = part_ref.at[pl.ds(pl.multiple_of((xp * NZ + zp) * per, per), per)]
            copy = pltpu.make_async_remote_copy(
                src_ref=src,
                dst_ref=recvx.at[n, o - 1],
                send_sem=sx.at[n, o - 1],
                recv_sem=rx.at[n, o - 1],
                device_id=(zi * NX + xp, cand, dp),
                device_id_type=MESH,
            )
            copy.start()
            row.append(copy)
        xcopies.append(row)

    tower(PLAN[1])

    zcopies = []
    pooled = None
    for n, k in enumerate(turns):
        zp = lax.rem(zi + k, NZ)
        for copy in xcopies[n]:
            copy.wait_recv()
        mine = part_ref[pl.ds(pl.multiple_of((xi * NZ + zp) * per, per), per), :]
        total = mine + recvx[n, 0] + recvx[n, 1] + recvx[n, 2]
        if k == 0:
            pooled = total
        else:
            sendz[k - 1] = total
            copy = pltpu.make_async_remote_copy(
                src_ref=sendz.at[k - 1],
                dst_ref=recvz.at[k - 1],
                send_sem=sz.at[k - 1],
                recv_sem=rz.at[k - 1],
                device_id=(zp * NX + xi, cand, dp),
                device_id_type=MESH,
            )
            copy.start()
            zcopies.append(copy)
    tower(PLAN[2])
    for copy in zcopies:
        copy.wait_recv()
    pooled = pooled + recvz[0] + recvz[1] + recvz[2]

    mine_at = pl.ds(pl.multiple_of(table * width, width), width)
    p0 = pooled.astype(bf16)
    rest = pooled - p0.astype(f32)
    p1 = rest.astype(bf16)
    p2 = (rest - p1.astype(f32)).astype(bf16)
    terms = jnp.dot(jnp.concatenate([p0, p1, p2], axis=0), weight_ref[mine_at, :], preferred_element_type=f32)
    terms = terms[:per] + terms[per : 2 * per] + terms[2 * per :]
    for b in range(groups):
        sendt[b] = terms[b * own : (b + 1) * own, :]

    for a in (2, 3, 1, 0):
        for k in (2, 1, 3, 0):
            if a or k:
                there, that = lax.rem(cand + a, ncand), lax.rem(dp + k, ndp)
                pltpu.make_async_remote_copy(
                    src_ref=sendt.at[there * ndp + that],
                    dst_ref=recvt.at[a * ndp + k - 1],
                    send_sem=st,
                    recv_sem=rt,
                    device_id=(tab, there, that),
                    device_id_type=MESH,
                ).start()

    tower(PLAN[3])
    all_t = pltpu.make_async_copy(recvt, recvt, rt)
    all_t.wait()
    total = sendt[table]
    for b in range(groups - 1):
        total = total + recvt[b]
    embed = unit_rows(total)
    embed_ref[...] = embed
    item_ref[...] = embed

    me = tab * ndp + dp

    for k in turns:

        @pl.loop(0 if k else 1, NX * ndp)
        def _(n):
            zp = lax.rem(zi + k, NZ)
            xp = lax.rem(xi + lax.div(n, ndp), NX)
            pltpu.make_async_remote_copy(
                src_ref=embed_ref,
                dst_ref=gathered.at[me],
                send_sem=sg,
                recv_sem=rg,
                device_id=(zp * NX + xp, cand, lax.rem(dp + n, ndp)),
                device_id_type=MESH,
            ).start()

    gathered[me] = embed
    tower(PLAN[4])
    most = gathered.at[pl.ds(0, ntab * ndp - 1)]
    pltpu.make_async_copy(most, most, rg).wait()

    pieces = [gathered[b] for b in range(ntab * ndp)]
    items = jnp.concatenate(pieces, axis=0)
    item_high, item_low = split2(items)
    dims = (((1,), (1,)), ((), ()))
    count = items.shape[0]

    def score(c, _):
        at = pl.ds(pl.multiple_of(c * USERS_AT_ONCE, USERS_AT_ONCE), USERS_AT_ONCE)
        high = high_ref[at, :]
        scores = (
            lax.dot_general(item_high, high, dims, preferred_element_type=f32)
            + lax.dot_general(item_low, high, dims, preferred_element_type=f32)
            + lax.dot_general(item_high, low_ref[at, :], dims, preferred_element_type=f32)
        )
        sums = jnp.sum(jnp.exp(scores), axis=0, keepdims=True)
        for h in range(USERS_AT_ONCE // 128):
            line = c * (USERS_AT_ONCE // 128) + h
            place = place_ref[pl.ds(line, 1), :]
            block = lax.shift_right_logical(place, 4)
            here = lax.rem(block, ncand) == cand
            row = jnp.where(here, lax.div(block, ncand) * 16 + (place & 15), -1)
            part = scores[:, h * 128 : (h + 1) * 128]
            positive = jnp.sum(
                jnp.where(iota((count, 128), 0) == row, part, f32(0.0)), axis=0, keepdims=True
            )
            stats[pl.ds(line, 1), :] = sums[:, h * 128 : (h + 1) * 128]
            stats[pl.ds(line + place_ref.shape[0], 1), :] = positive
        return 0

    lax.fori_loop(0, xv.shape[0] // USERS_AT_ONCE, score, 0, unroll=4)

    scopies = []
    for o in range(1, ncand):
        copy = pltpu.make_async_remote_copy(
            src_ref=stats,
            dst_ref=others.at[o - 1],
            send_sem=ss.at[o - 1],
            recv_sem=rs.at[o - 1],
            device_id=(tab, lax.rem(cand + o, ncand), dp),
            device_id_type=MESH,
        )
        copy.start()
        scopies.append(copy)
    for row in xcopies:
        for copy in row:
            copy.wait_send()
    for copy in zcopies:
        copy.wait_send()
    pltpu.make_async_copy(recvt, recvt, st).wait()
    pltpu.make_async_copy(most, most, sg).wait()
    for copy in scopies:
        copy.wait_recv()
    both = stats[...] + others[0] + others[1] + others[2]
    lines = place_ref.shape[0]
    loss_ref[...] = jnp.log(both[:lines]) - both[lines:]
    for copy in scopies:
        copy.wait_send()


def step(flat, extra, lengths, table, item_weight, features, user_w1, user_w2, places):
    items, width = extra.shape
    rows = table.shape[0]
    users, embed = features.shape[0], user_w2.shape[1]
    per = items // (NX * NZ)
    own = per // 16
    lines = users // 128
    vmem = pl.BlockSpec(memory_space=pltpu.VMEM)
    hbm = pl.BlockSpec(memory_space=pltpu.HBM)
    dma = pltpu.SemaphoreType.DMA
    return pl.pallas_call(
        step_kernel,
        name="step",
        out_shape=(jax.ShapeDtypeStruct((own, embed), f32), jax.ShapeDtypeStruct((lines, 128), f32)),
        in_specs=[pl.BlockSpec(memory_space=pltpu.SMEM), vmem, vmem, vmem, hbm, *[vmem] * 5],
        out_specs=(vmem, vmem),
        scratch_shapes=[
            pltpu.VMEM((rows, width), bf16),
            pltpu.VMEM((rows, width), f32),
            pltpu.VMEM((CAPACITY, width), f32),
            pltpu.VMEM((items, width), f32),
            pltpu.VMEM((users, embed), bf16),
            pltpu.VMEM((users, embed), bf16),
            pltpu.VMEM((NZ, NX - 1, per, width), f32),
            pltpu.VMEM((NZ - 1, per, width), f32),
            pltpu.VMEM((NZ - 1, per, width), f32),
            pltpu.VMEM((16, own, embed), f32),
            pltpu.VMEM((15, own, embed), f32),
            pltpu.VMEM((own, embed), f32),
            pltpu.VMEM((64, own, embed), f32),
            pltpu.VMEM((2 * lines, 128), f32),
            pltpu.VMEM((3, 2 * lines, 128), f32),
            dma((CHUNKS,)),
            dma((NZ, NX - 1)),
            dma((NZ, NX - 1)),
            dma((NZ - 1,)),
            dma((NZ - 1,)),
            dma,
            dma,
            dma,
            dma,
            dma((3,)),
            dma((3,)),
        ],
        compiler_params=pltpu.CompilerParams(
            collective_id=0, has_side_effects=True, vmem_limit_bytes=46 * 2**20
        ),
        cost_estimate=pl.CostEstimate(flops=5 * 10**9, bytes_accessed=5 * 2**20, transcendentals=0),
    )(flat, flat, extra, lengths, table, item_weight, features, user_w1, user_w2, places)


def body(
    tables, bag_ids, bag_lengths, item_weight, user_features, user_w1, user_w2, positive_items
):
    flat, extra = make_list(bag_ids[0].T, bag_lengths, tables[0])
    item_emb, loss = step(
        flat, extra, bag_lengths, tables[0], item_weight, user_features, user_w1, user_w2, positive_items.reshape(-1, 128)
    )
    return (item_emb, loss.reshape(-1))


def solution(mesh):
    placed = (
        P(("cand", "dp"), "tab", None),
        P(("cand", "dp"), None, None),
        P(("cand", "dp"), None),
        P(),
        P(("tab", "dp"), None),
        P(),
        P(),
        P(("tab", "dp")),
    )
    return jax.shard_map(
        body,
        mesh=mesh,
        in_specs=placed,
        out_specs=(P(("tab", "cand", "dp"), None), P(("tab", "dp"))),
        check_vma=False,
    )
```

```python
import functools
import jax
import jax.numpy as jnp
from jax import lax
from jax.experimental import pallas as pl
from jax.experimental.pallas import tpu as pltpu
from jax.sharding import PartitionSpec as P

MESH = pl.DeviceIdType.MESH
f32, bf16, i32 = jnp.float32, jnp.bfloat16, jnp.int32
epsilon = 1e-06
logit_scale = 20.0
NX, NZ = 4, 4
PARTS = 4
DEPTH = 16
CHUNKS = 8
CAPACITY = 704
LINES = 6
LANE_DEPTH = 20


def iota(shape, dim):
    return lax.broadcasted_iota(i32, shape, dim)


def list_kernel(ids_ref, table_ref, list_out, extra_ref, stage, tab, acc0, acc1, acc2, acc3,
                rank_ref, code_ref, list_ref, slist, load_sems, list_sem):
    rows = table_ref.shape[0]
    positions, items = ids_ref.shape
    tiles = items // 128
    chunk = rows // CHUNKS
    base = lax.axis_index("tab") * rows
    accs = (acc0, acc1, acc2, acc3)

    slots = tiles * positions
    ids = jnp.concatenate([ids_ref[:, 128 * t : 128 * (t + 1)] for t in range(tiles)], axis=0)
    r = iota((slots, 128), 0)
    lane = iota((slots, 128), 1)
    local = ids - base
    live = (local >= 0) & (local < rows)
    item = lax.div(r, positions) * 128 + lane
    per = items // (NX * NZ)
    block = lax.div(item, per)
    dest = (lax.rem(block, NX) * NZ + lax.div(block, NX)) * per + lax.rem(item, per)
    code = local * 2048 + dest + 1
    below = jnp.where(iota((slots, slots), 0) >= iota((slots, slots), 1), f32(1.0), f32(0.0)).astype(bf16)
    ones = jnp.ones((128, 128), bf16)

    def ordered(which):
        marks = jnp.where(which, f32(1.0), f32(0.0)).astype(bf16)
        order = jnp.dot(below, marks, preferred_element_type=f32)
        return order, jnp.where(which, order - 1.0, f32(-1.0)).astype(i32)

    order, rank = ordered(live)
    counts = jnp.minimum(order[slots - 1 : slots, :], f32(LANE_DEPTH))
    square = (128, 128)
    before = iota(square, 0) < iota(square, 1)
    offset = jnp.dot(
        jnp.broadcast_to(counts, (8, 128)).astype(bf16),
        jnp.where(before, f32(1.0), f32(0.0)).astype(bf16),
        preferred_element_type=f32,
    )
    spread = jnp.broadcast_to(counts, square)
    after = iota(square, 0) > iota(square, 1)
    eye = iota(square, 0) == iota(square, 1)
    column = jnp.dot(
        jnp.concatenate([jnp.where(after, spread, f32(0.0)), jnp.where(eye, spread, f32(0.0))], axis=0).astype(bf16),
        ones,
        preferred_element_type=f32,
    )
    offset_column, count_column = column[:128].astype(i32), column[128:].astype(i32)
    offset_row = offset[:1].astype(i32)
    lane_square = iota(square, 1)
    lines = iota((8, 128), 0)
    left, right = [], []
    for k in range(LANE_DEPTH):
        found = jnp.sum(jnp.where(rank == k, code, 0), axis=0, keepdims=True)
        where_to = jnp.broadcast_to(lax.shift_right_logical(offset_row + k, 7), (8, 128)) == lines
        left.append(
            jnp.concatenate(
                [
                    jnp.where(where_to, jnp.broadcast_to(lax.shift_right_logical(found, 7 * p) & 127, (8, 128)), 0)
                    for p in range(4)
                ],
                axis=0,
            ).astype(f32).astype(bf16)
        )
        hit = (((offset_column + k) & 127) == lane_square) & (count_column > k)
        right.append(jnp.where(hit, f32(1.0), f32(0.0)).astype(bf16))
    flat = jnp.dot(
        jnp.concatenate(left, axis=1), jnp.concatenate(right, axis=0), preferred_element_type=f32
    ).astype(i32)
    codes = flat[:8] + flat[8:16] * 128 + flat[16:24] * 16384 + flat[24:32] * 2097152
    list_out[:8, :] = lax.shift_right_logical(codes, 11)
    list_out[8:, :] = codes & 2047
    extra_ref[...] = jnp.zeros_like(extra_ref)

    place = offset_row + rank
    over = live & ((rank >= LANE_DEPTH) | (place >= CAPACITY))
    beyond = jnp.max(jnp.where(over, f32(1.0), f32(0.0)))

    @pl.when(beyond > 0.0)
    def _():
        loads = [
            pltpu.make_async_copy(
                table_ref.at[pl.ds(c * chunk, chunk)], stage.at[pl.ds(c * chunk, chunk)], load_sems.at[c]
            )
            for c in range(CHUNKS)
        ]
        for load in loads:
            load.start()
        order, rank = ordered(over)
        rank_ref[...] = rank
        code_ref[...] = code
        counts = order[slots - 1 : slots, :].astype(i32)
        most = jnp.max(counts)
        for acc in accs:
            acc[...] = jnp.zeros_like(acc)
        for load in loads:
            load.wait()

        @pl.loop(0, rows // 256)
        def _(s):
            at = pl.ds(pl.multiple_of(s * 256, 256), 256)
            tab[at, :] = stage[at, :].astype(f32)

        def more(b, _):
            for k in range(DEPTH):
                found = jnp.sum(
                    jnp.where(rank_ref[...] == b * DEPTH + k, code_ref[...], 0), axis=0, keepdims=True
                )
                list_ref[k : k + 1, :] = found
            list_ref[DEPTH : DEPTH + 1, :] = jnp.clip(counts - b * DEPTH, 0, DEPTH)
            copy = pltpu.make_async_copy(list_ref, slist, list_sem)
            copy.start()
            copy.wait()

            @pl.loop(0, 128)
            def _(at):
                def group(g, _):
                    for q in range(PARTS):
                        code = slist[g * PARTS + q, at]
                        row = lax.shift_right_logical(code, 11)
                        to = code & 2047
                        accs[q][pl.ds(to, 1), :] += tab[pl.ds(row, 1), :]
                    return 0

                lax.fori_loop(0, lax.shift_right_logical(slist[DEPTH, at] + PARTS - 1, 2), group, 0)

            return 0

        lax.fori_loop(0, lax.div(most + DEPTH - 1, DEPTH), more, 0)
        extra_ref[...] = acc0[1 : items + 1, :] + acc1[1 : items + 1, :] + acc2[1 : items + 1, :] + acc3[1 : items + 1, :]


def make_list(ids_t, table):
    rows, width = table.shape
    positions, items = ids_t.shape
    slots = positions * items // 128
    vmem = pl.BlockSpec(memory_space=pltpu.VMEM)
    return pl.pallas_call(
        list_kernel,
        name="list",
        out_shape=(jax.ShapeDtypeStruct((16, 128), i32), jax.ShapeDtypeStruct((items, width), f32)),
        in_specs=[vmem, pl.BlockSpec(memory_space=pltpu.HBM)],
        out_specs=(vmem, vmem),
        scratch_shapes=[
            pltpu.VMEM((rows, width), bf16),
            pltpu.VMEM((rows, width), f32),
            *[pltpu.VMEM((items + 8, width), f32)] * PARTS,
            pltpu.VMEM((slots, 128), i32),
            pltpu.VMEM((slots, 128), i32),
            pltpu.VMEM((DEPTH + 8, 128), i32),
            pltpu.SMEM((DEPTH + 8, 128), i32),
            pltpu.SemaphoreType.DMA((CHUNKS,)),
            pltpu.SemaphoreType.DMA,
        ],
        compiler_params=pltpu.CompilerParams(vmem_limit_bytes=52 * 2**20),
        cost_estimate=pl.CostEstimate(flops=10**8, bytes_accessed=2**20, transcendentals=0),
    )(ids_t, table)


def split2(v):
    high = v.astype(bf16)
    return high, (v - high.astype(f32)).astype(bf16)


def unit_rows(v):
    return v * lax.rsqrt(jnp.mean(v * v, axis=-1, keepdims=True) + epsilon)


PLAN = (0, 3, 1, 1, 3)
USERS_AT_ONCE = 256
TOGETHER = 16
UNROLL = 4


def step_kernel(vlist, extra_ref, len_ref, table_ref, weight_ref, x_ref, w1_ref, w2_ref, place_ref, item_ref, loss_ref,
                stage, wide, listed, part_ref, xv, w1v, w2v, wv, high_ref, low_ref, recvx, sendz, recvz, sendt, recvt, embed_ref,
                gathered, stats, others, slist, list_sem, table_sems, load_sems, sx, rx, sz, rz, st, rt, sg, rg, ss, rs):
    tab, cand, dp = lax.axis_index("tab"), lax.axis_index("cand"), lax.axis_index("dp")
    xi, zi = lax.rem(tab, NX), lax.div(tab, NX)
    ntab, ncand, ndp = NX * NZ, 4, 4
    width = part_ref.shape[1]
    per = part_ref.shape[0] // ntab
    groups = ncand * ndp
    own = per // groups
    table = cand * ndp + dp

    list_copy = pltpu.make_async_copy(vlist.at[pl.ds(0, 8)], slist, list_sem)
    list_copy.start()

    def local(src, dst, k):
        return pltpu.make_async_copy(src, dst, load_sems.at[k])

    rows = table_ref.shape[0]
    chunk = rows // CHUNKS
    table_loads = []
    for c in range(CHUNKS):
        at = pl.ds(c * chunk, chunk)
        table_loads.append(pltpu.make_async_copy(table_ref.at[at], stage.at[at], table_sems.at[c]))
        table_loads[-1].start()

    loads = [
        local(x_ref, xv, 0),
        local(w1_ref, w1v, 1),
        local(w2_ref, w2v, 2),
        local(weight_ref.at[pl.ds(pl.multiple_of(table * width, width), width)], wv, 3),
    ]

    barrier = pltpu.get_barrier_semaphore()

    def greet(device):
        pl.semaphore_signal(barrier, inc=1, device_id=device, device_id_type=MESH)

    for a in (2, 3, 1, 0):
        for k in (2, 1, 3, 0):
            if a or k:
                greet((tab, lax.rem(cand + a, ncand), lax.rem(dp + k, ndp)))
    for k in range(1, NZ):
        greet((lax.rem(zi + k, NZ) * NX + xi, cand, dp))
    for k in range(1, NX):
        greet((zi * NX + lax.rem(xi + k, NX), cand, dp))

    done = [0]

    def tower(chunks):
        if done[0] == 0:
            for k in range(3):
                loads[k].wait()
        first = done[0]
        done[0] += chunks

        @pl.loop(first, first + chunks)
        def _(c):
            at = pl.ds(pl.multiple_of(c * USERS_AT_ONCE, USERS_AT_ONCE), USERS_AT_ONCE)
            hidden = jnp.dot(xv[at, :], w1v[...], preferred_element_type=f32)
            hidden = (0.5 * hidden * (1.0 + lax.erf(hidden * f32(0.5**0.5)))).astype(bf16)
            users = unit_rows(jnp.dot(hidden, w2v[...], preferred_element_type=f32))
            high, low = split2((users * (logit_scale / users.shape[1])).T)
            high_ref[:, at] = high
            low_ref[:, at] = low

    for c in range(CHUNKS):
        table_loads[c].wait()
        if c == CHUNKS - 2:
            for load in loads:
                load.start()

        @pl.loop(0, chunk // 256)
        def _(s):
            at = pl.ds(pl.multiple_of(c * chunk + s * 256, 256), 256)
            wide[at, :] = stage[at, :].astype(f32)

    list_copy.wait()
    listed[CAPACITY:, :] = jnp.zeros_like(listed[CAPACITY:, :])
    for line in range(LINES):

        @pl.loop(0, min(128, CAPACITY - 128 * line) // TOGETHER)
        def _(g):
            at = pl.multiple_of(g * TOGETHER, TOGETHER)
            fetched = []
            for q in range(TOGETHER):
                fetched.append(wide[pl.ds(slist[line, at + q], 1), :])
            for q in range(TOGETHER):
                listed[pl.ds(line * 128 + at + q, 1), :] = fetched[q]

    square = (128, 128)
    eye = iota(square, 0) == iota(square, 1)
    ones = jnp.ones(square, bf16)
    picked = listed[...].astype(bf16)
    wanted = vlist[8:, :]
    for b in range(part_ref.shape[0] // 128):
        select = jnp.concatenate(
            [
                jnp.where(wanted[n : n + 1, :] == iota(square, 0) + (128 * b + 1), f32(1.0), f32(0.0)).astype(bf16)
                for n in range(LINES)
            ],
            axis=1,
        )
        ends = []
        for h in range(128 // per):
            to = b * (128 // per) + h
            t = (to % NZ) * NX + to // NZ
            ends.append(len_ref[:, t * per : (t + 1) * per])
        spread = jnp.broadcast_to(jnp.concatenate(ends, axis=1).astype(f32), square)
        column = jnp.dot(jnp.where(eye, spread, f32(0.0)).astype(bf16), ones, preferred_element_type=f32)
        at = pl.ds(128 * b, 128)
        part_ref[at, :] = (jnp.dot(select, picked, preferred_element_type=f32) + extra_ref[at, :]) / column

    if PLAN[0]:
        tower(PLAN[0])
    pl.semaphore_wait(barrier, groups - 1 + NZ - 1 + NX - 1)

    xcopies = []
    turns = (2, 1, 3, 0)
    for n, k in enumerate(turns):
        zp = lax.rem(zi + k, NZ)
        row = []
        for o in range(1, NX):
            xp = lax.rem(xi + o, NX)
            src = part_ref.at[pl.ds(pl.multiple_of((xp * NZ + zp) * per, per), per)]
            copy = pltpu.make_async_remote_copy(
                src_ref=src,
                dst_ref=recvx.at[n, o - 1],
                send_sem=sx.at[n, o - 1],
                recv_sem=rx.at[n, o - 1],
                device_id=(zi * NX + xp, cand, dp),
                device_id_type=MESH,
            )
            copy.start()
            row.append(copy)
        xcopies.append(row)

    tower(PLAN[1])

    zcopies = []
    pooled = None
    for n, k in enumerate(turns):
        zp = lax.rem(zi + k, NZ)
        for copy in xcopies[n]:
            copy.wait_recv()
        mine = part_ref[pl.ds(pl.multiple_of((xi * NZ + zp) * per, per), per), :]
        total = mine + recvx[n, 0] + recvx[n, 1] + recvx[n, 2]
        if k == 0:
            pooled = total
        else:
            sendz[k - 1] = total
            copy = pltpu.make_async_remote_copy(
                src_ref=sendz.at[k - 1],
                dst_ref=recvz.at[k - 1],
                send_sem=sz.at[k - 1],
                recv_sem=rz.at[k - 1],
                device_id=(zp * NX + xi, cand, dp),
                device_id_type=MESH,
            )
            copy.start()
            zcopies.append(copy)
    tower(PLAN[2])
    loads[3].wait()
    for copy in zcopies:
        copy.wait_recv()
    pooled = pooled + recvz[0] + recvz[1] + recvz[2]

    p0 = pooled.astype(bf16)
    rest = pooled - p0.astype(f32)
    p1 = rest.astype(bf16)
    p2 = (rest - p1.astype(f32)).astype(bf16)
    terms = jnp.dot(jnp.concatenate([p0, p1, p2], axis=0), wv[...], preferred_element_type=f32)
    terms = terms[:per] + terms[per : 2 * per] + terms[2 * per :]
    for b in range(groups):
        sendt[b] = terms[b * own : (b + 1) * own, :]

    for a in (2, 3, 1, 0):
        for k in (2, 1, 3, 0):
            if a or k:
                there, that = lax.rem(cand + a, ncand), lax.rem(dp + k, ndp)
                pltpu.make_async_remote_copy(
                    src_ref=sendt.at[there * ndp + that],
                    dst_ref=recvt.at[a * ndp + k - 1],
                    send_sem=st,
                    recv_sem=rt,
                    device_id=(tab, there, that),
                    device_id_type=MESH,
                ).start()

    tower(PLAN[3])
    all_t = pltpu.make_async_copy(recvt, recvt, rt)
    all_t.wait()
    total = sendt[table]
    for b in range(groups - 1):
        total = total + recvt[b]
    embed = unit_rows(total)
    embed_ref[...] = embed
    item_ref[...] = embed

    me = tab * ndp + dp

    for k in turns:

        @pl.loop(0 if k else 1, NX * ndp)
        def _(n):
            zp = lax.rem(zi + k, NZ)
            xp = lax.rem(xi + lax.div(n, ndp), NX)
            pltpu.make_async_remote_copy(
                src_ref=embed_ref,
                dst_ref=gathered.at[me],
                send_sem=sg,
                recv_sem=rg.at[lax.rem(lax.div(zp, 2) + lax.div(zi, 2), 2)],
                device_id=(zp * NX + xp, cand, lax.rem(dp + n, ndp)),
                device_id_type=MESH,
            ).start()

    gathered[me] = embed
    tower(PLAN[4])
    lines = place_ref.shape[0]
    half = ntab * ndp // 2

    def add_scores(side, first):
        pieces = [gathered[side * half + b] for b in range(half)]
        items = jnp.concatenate(pieces, axis=0)
        item_high, item_low = split2(items)
        count = items.shape[0]
        stacked = jnp.concatenate([item_high, item_low], axis=0)

        def score(c, _):
            at = pl.ds(pl.multiple_of(c * USERS_AT_ONCE, USERS_AT_ONCE), USERS_AT_ONCE)
            both = jnp.dot(stacked, high_ref[:, at], preferred_element_type=f32)
            rest = jnp.dot(item_high, low_ref[:, at], preferred_element_type=f32)
            scores = both[:count] + both[count:] + rest
            sums = jnp.sum(jnp.exp(scores), axis=0, keepdims=True)
            for h in range(USERS_AT_ONCE // 128):
                line = c * (USERS_AT_ONCE // 128) + h
                place = place_ref[pl.ds(line, 1), :]
                block = lax.shift_right_logical(place, 4)
                here = lax.rem(block, ncand) == cand
                row = jnp.where(here, lax.div(block, ncand) * 16 + (place & 15) - side * count, -1)
                part = scores[:, h * 128 : (h + 1) * 128]
                positive = jnp.sum(
                    jnp.where(iota((count, 128), 0) == row, part, f32(0.0)), axis=0, keepdims=True
                )
                total = sums[:, h * 128 : (h + 1) * 128]
                if not first:
                    total = total + stats[pl.ds(line, 1), :]
                    positive = positive + stats[pl.ds(line + lines, 1), :]
                stats[pl.ds(line, 1), :] = total
                stats[pl.ds(line + lines, 1), :] = positive
            return 0

        lax.fori_loop(0, high_ref.shape[1] // USERS_AT_ONCE, score, 0, unroll=UNROLL)

    most = gathered.at[pl.ds(0, ntab * ndp - 1)]
    near = gathered.at[pl.ds(0, half - 1)]
    far = gathered.at[pl.ds(0, half)]
    side = lax.div(zi, 2)
    pltpu.make_async_copy(near, near, rg.at[0]).wait()
    add_scores(side, True)
    pltpu.make_async_copy(far, far, rg.at[1]).wait()
    add_scores(1 - side, False)

    scopies = []
    for o in range(1, ncand):
        copy = pltpu.make_async_remote_copy(
            src_ref=stats,
            dst_ref=others.at[o - 1],
            send_sem=ss.at[o - 1],
            recv_sem=rs.at[o - 1],
            device_id=(tab, lax.rem(cand + o, ncand), dp),
            device_id_type=MESH,
        )
        copy.start()
        scopies.append(copy)
    for row in xcopies:
        for copy in row:
            copy.wait_send()
    for copy in zcopies:
        copy.wait_send()
    pltpu.make_async_copy(recvt, recvt, st).wait()
    pltpu.make_async_copy(most, most, sg).wait()
    for copy in scopies:
        copy.wait_recv()
    both = stats[...] + others[0] + others[1] + others[2]
    loss_ref[...] = jnp.log(both[:lines]) - both[lines:]
    for copy in scopies:
        copy.wait_send()


def step(flat, extra, lengths, table, item_weight, features, user_w1, user_w2, places):
    items, width = extra.shape
    rows = table.shape[0]
    users, features_in = features.shape
    hidden, embed = user_w2.shape
    per = items // (NX * NZ)
    own = per // 16
    lines = users // 128
    vmem = pl.BlockSpec(memory_space=pltpu.VMEM)
    hbm = pl.BlockSpec(memory_space=pltpu.HBM)
    dma = pltpu.SemaphoreType.DMA
    return pl.pallas_call(
        step_kernel,
        name="step",
        out_shape=(jax.ShapeDtypeStruct((own, embed), f32), jax.ShapeDtypeStruct((lines, 128), f32)),
        in_specs=[vmem, vmem, vmem, hbm, hbm, hbm, hbm, hbm, vmem],
        out_specs=(vmem, vmem),
        scratch_shapes=[
            pltpu.VMEM((rows, width), bf16),
            pltpu.VMEM((rows, width), f32),
            pltpu.VMEM((128 * LINES, width), f32),
            pltpu.VMEM((items, width), f32),
            pltpu.VMEM((users, features_in), bf16),
            pltpu.VMEM((features_in, hidden), bf16),
            pltpu.VMEM((hidden, embed), bf16),
            pltpu.VMEM((width, embed), bf16),
            pltpu.VMEM((embed, users), bf16),
            pltpu.VMEM((embed, users), bf16),
            pltpu.VMEM((NZ, NX - 1, per, width), f32),
            pltpu.VMEM((NZ - 1, per, width), f32),
            pltpu.VMEM((NZ - 1, per, width), f32),
            pltpu.VMEM((16, own, embed), f32),
            pltpu.VMEM((15, own, embed), f32),
            pltpu.VMEM((own, embed), f32),
            pltpu.VMEM((64, own, embed), f32),
            pltpu.VMEM((2 * lines, 128), f32),
            pltpu.VMEM((3, 2 * lines, 128), f32),
            pltpu.SMEM((8, 128), i32),
            dma,
            dma((CHUNKS,)),
            dma((4,)),
            dma((NZ, NX - 1)),
            dma((NZ, NX - 1)),
            dma((NZ - 1,)),
            dma((NZ - 1,)),
            dma,
            dma,
            dma,
            dma((2,)),
            dma((3,)),
            dma((3,)),
        ],
        compiler_params=pltpu.CompilerParams(
            collective_id=0, has_side_effects=True, vmem_limit_bytes=52 * 2**20
        ),
        cost_estimate=pl.CostEstimate(flops=5 * 10**9, bytes_accessed=5 * 2**20, transcendentals=0),
    )(flat, extra, lengths, table, item_weight, features, user_w1, user_w2, places)


def finish_kernel(item_ref, loss_ref, item_out, loss_out):
    item_out[...] = item_ref[...]
    loss_out[...] = loss_ref[...]


def finish(item_emb, loss):
    vmem = pl.BlockSpec(memory_space=pltpu.VMEM)
    return pl.pallas_call(
        finish_kernel,
        name="finish",
        out_shape=(
            jax.ShapeDtypeStruct(item_emb.shape, f32),
            jax.ShapeDtypeStruct(loss.shape, f32),
        ),
        in_specs=[vmem, vmem],
        out_specs=(vmem, vmem),
        compiler_params=pltpu.CompilerParams(vmem_limit_bytes=2**20),
    )(item_emb, loss)


def body(
    tables, bag_ids, bag_lengths, item_weight, user_features, user_w1, user_w2, positive_items
):
    ids = bag_ids[0].T
    ids = jnp.where(iota(ids.shape, 0) < bag_lengths, ids, i32(-1))
    flat, extra = make_list(ids, tables[0])
    item_emb, loss = step(
        flat, extra, bag_lengths, tables[0], item_weight, user_features, user_w1, user_w2, positive_items.reshape(-1, 128)
    )
    item_emb, loss = finish(item_emb, loss)
    return (item_emb, loss.reshape(-1))


def solution(mesh):
    placed = (
        P(("cand", "dp"), "tab", None),
        P(("cand", "dp"), None, None),
        P(("cand", "dp"), None),
        P(),
        P(("tab", "dp"), None),
        P(),
        P(),
        P(("tab", "dp")),
    )
    return jax.shard_map(
        body,
        mesh=mesh,
        in_specs=placed,
        out_specs=(P(("tab", "cand", "dp"), None), P(("tab", "dp"))),
        check_vma=False,
    )
```

```python
import functools
import jax
import jax.numpy as jnp
from jax import lax
from jax.experimental import pallas as pl
from jax.experimental.pallas import tpu as pltpu
from jax.sharding import PartitionSpec as P

MESH = pl.DeviceIdType.MESH
f32, bf16, i32 = jnp.float32, jnp.bfloat16, jnp.int32
epsilon = 1e-06
logit_scale = 20.0
NX, NZ = 4, 4
PARTS = 4
DEPTH = 16
CHUNKS = 8
CAPACITY = 704
LINES = 6
LANE_DEPTH = 20


def iota(shape, dim):
    return lax.broadcasted_iota(i32, shape, dim)


def list_kernel(ids_ref, table_ref, list_out, extra_ref, stage, tab, acc0, acc1, acc2, acc3,
                rank_ref, code_ref, list_ref, slist, load_sems, list_sem):
    rows = table_ref.shape[0]
    positions, items = ids_ref.shape
    tiles = items // 128
    chunk = rows // CHUNKS
    base = lax.axis_index("tab") * rows
    accs = (acc0, acc1, acc2, acc3)

    slots = tiles * positions
    ids = jnp.concatenate([ids_ref[:, 128 * t : 128 * (t + 1)] for t in range(tiles)], axis=0)
    r = iota((slots, 128), 0)
    lane = iota((slots, 128), 1)
    local = ids - base
    live = (local >= 0) & (local < rows)
    item = lax.div(r, positions) * 128 + lane
    code = local * 2048 + item + 1
    below = jnp.where(iota((slots, slots), 0) >= iota((slots, slots), 1), f32(1.0), f32(0.0)).astype(bf16)
    ones = jnp.ones((128, 128), bf16)

    def ordered(which):
        marks = jnp.where(which, f32(1.0), f32(0.0)).astype(bf16)
        order = jnp.dot(below, marks, preferred_element_type=f32)
        return order, jnp.where(which, order - 1.0, f32(-1.0)).astype(i32)

    order, rank = ordered(live)
    counts = jnp.minimum(order[slots - 1 : slots, :], f32(LANE_DEPTH))
    square = (128, 128)
    before = iota(square, 0) < iota(square, 1)
    offset = jnp.dot(
        jnp.broadcast_to(counts, (8, 128)).astype(bf16),
        jnp.where(before, f32(1.0), f32(0.0)).astype(bf16),
        preferred_element_type=f32,
    )
    spread = jnp.broadcast_to(counts, square)
    after = iota(square, 0) > iota(square, 1)
    eye = iota(square, 0) == iota(square, 1)
    column = jnp.dot(
        jnp.concatenate([jnp.where(after, spread, f32(0.0)), jnp.where(eye, spread, f32(0.0))], axis=0).astype(bf16),
        ones,
        preferred_element_type=f32,
    )
    offset_column, count_column = column[:128].astype(i32), column[128:].astype(i32)
    offset_row = offset[:1].astype(i32)
    lane_square = iota(square, 1)
    lines = iota((8, 128), 0)
    left, right = [], []
    for k in range(LANE_DEPTH):
        found = jnp.sum(jnp.where(rank == k, code, 0), axis=0, keepdims=True)
        where_to = jnp.broadcast_to(lax.shift_right_logical(offset_row + k, 7), (8, 128)) == lines
        left.append(
            jnp.concatenate(
                [
                    jnp.where(where_to, jnp.broadcast_to(lax.shift_right_logical(found, 7 * p) & 127, (8, 128)), 0)
                    for p in range(4)
                ],
                axis=0,
            ).astype(f32).astype(bf16)
        )
        hit = (((offset_column + k) & 127) == lane_square) & (count_column > k)
        right.append(jnp.where(hit, f32(1.0), f32(0.0)).astype(bf16))
    flat = jnp.dot(
        jnp.concatenate(left, axis=1), jnp.concatenate(right, axis=0), preferred_element_type=f32
    ).astype(i32)
    codes = flat[:8] + flat[8:16] * 128 + flat[16:24] * 16384 + flat[24:32] * 2097152
    list_out[:8, :] = lax.shift_right_logical(codes, 11)
    list_out[8:, :] = codes & 2047
    extra_ref[...] = jnp.zeros_like(extra_ref)

    place = offset_row + rank
    over = live & ((rank >= LANE_DEPTH) | (place >= CAPACITY))
    beyond = jnp.max(jnp.where(over, f32(1.0), f32(0.0)))

    @pl.when(beyond > 0.0)
    def _():
        loads = [
            pltpu.make_async_copy(
                table_ref.at[pl.ds(c * chunk, chunk)], stage.at[pl.ds(c * chunk, chunk)], load_sems.at[c]
            )
            for c in range(CHUNKS)
        ]
        for load in loads:
            load.start()
        order, rank = ordered(over)
        rank_ref[...] = rank
        code_ref[...] = code
        counts = order[slots - 1 : slots, :].astype(i32)
        most = jnp.max(counts)
        for acc in accs:
            acc[...] = jnp.zeros_like(acc)
        for load in loads:
            load.wait()

        @pl.loop(0, rows // 256)
        def _(s):
            at = pl.ds(pl.multiple_of(s * 256, 256), 256)
            tab[at, :] = stage[at, :].astype(f32)

        def more(b, _):
            for k in range(DEPTH):
                found = jnp.sum(
                    jnp.where(rank_ref[...] == b * DEPTH + k, code_ref[...], 0), axis=0, keepdims=True
                )
                list_ref[k : k + 1, :] = found
            list_ref[DEPTH : DEPTH + 1, :] = jnp.clip(counts - b * DEPTH, 0, DEPTH)
            copy = pltpu.make_async_copy(list_ref, slist, list_sem)
            copy.start()
            copy.wait()

            @pl.loop(0, 128)
            def _(at):
                def group(g, _):
                    for q in range(PARTS):
                        code = slist[g * PARTS + q, at]
                        row = lax.shift_right_logical(code, 11)
                        to = code & 2047
                        accs[q][pl.ds(to, 1), :] += tab[pl.ds(row, 1), :]
                    return 0

                lax.fori_loop(0, lax.shift_right_logical(slist[DEPTH, at] + PARTS - 1, 2), group, 0)

            return 0

        lax.fori_loop(0, lax.div(most + DEPTH - 1, DEPTH), more, 0)
        extra_ref[...] = acc0[1 : items + 1, :] + acc1[1 : items + 1, :] + acc2[1 : items + 1, :] + acc3[1 : items + 1, :]


def make_list(ids_t, table):
    rows, width = table.shape
    positions, items = ids_t.shape
    slots = positions * items // 128
    vmem = pl.BlockSpec(memory_space=pltpu.VMEM)
    return pl.pallas_call(
        list_kernel,
        name="list",
        out_shape=(jax.ShapeDtypeStruct((16, 128), i32), jax.ShapeDtypeStruct((items, width), f32)),
        in_specs=[vmem, pl.BlockSpec(memory_space=pltpu.HBM)],
        out_specs=(vmem, vmem),
        scratch_shapes=[
            pltpu.VMEM((rows, width), bf16),
            pltpu.VMEM((rows, width), f32),
            *[pltpu.VMEM((items + 8, width), f32)] * PARTS,
            pltpu.VMEM((slots, 128), i32),
            pltpu.VMEM((slots, 128), i32),
            pltpu.VMEM((DEPTH + 8, 128), i32),
            pltpu.SMEM((DEPTH + 8, 128), i32),
            pltpu.SemaphoreType.DMA((CHUNKS,)),
            pltpu.SemaphoreType.DMA,
        ],
        compiler_params=pltpu.CompilerParams(vmem_limit_bytes=52 * 2**20),
        cost_estimate=pl.CostEstimate(flops=10**8, bytes_accessed=2**20, transcendentals=0),
    )(ids_t, table)


def split2(v):
    high = v.astype(bf16)
    return high, (v - high.astype(f32)).astype(bf16)


def unit_rows(v):
    return v * lax.rsqrt(jnp.mean(v * v, axis=-1, keepdims=True) + epsilon)


PLAN = (0, 3, 1, 1, 3)
USERS_AT_ONCE = 256
TOGETHER = 16
UNROLL = 4


def step_kernel(vlist, extra_ref, len_ref, table_ref, weight_ref, x_ref, w1_ref, w2_ref, place_ref, item_ref, loss_ref,
                stage, wide, listed, part_ref, columns, xv, w1v, w2v, wv, high_ref, low_ref, recvx, sendz, recvz, sendt, recvt, embed_ref,
                gathered, stats, others, slist, list_sem, table_sems, load_sems, sx, rx, sz, rz, st, rt, sg, rg, ss, rs):
    tab, cand, dp = lax.axis_index("tab"), lax.axis_index("cand"), lax.axis_index("dp")
    xi, zi = lax.rem(tab, NX), lax.div(tab, NX)
    ntab, ncand, ndp = NX * NZ, 4, 4
    width = part_ref.shape[1]
    per = part_ref.shape[0] // ntab
    groups = ncand * ndp
    own = per // groups
    table = cand * ndp + dp

    list_copy = pltpu.make_async_copy(vlist.at[pl.ds(0, 8)], slist, list_sem)
    list_copy.start()

    def local(src, dst, k):
        return pltpu.make_async_copy(src, dst, load_sems.at[k])

    rows = table_ref.shape[0]
    chunk = rows // CHUNKS
    table_loads = []
    for c in range(CHUNKS):
        at = pl.ds(c * chunk, chunk)
        table_loads.append(pltpu.make_async_copy(table_ref.at[at], stage.at[at], table_sems.at[c]))
        table_loads[-1].start()

    loads = [
        local(x_ref, xv, 0),
        local(w1_ref, w1v, 1),
        local(w2_ref, w2v, 2),
        local(weight_ref.at[pl.ds(pl.multiple_of(table * width, width), width)], wv, 3),
    ]

    barrier = pltpu.get_barrier_semaphore()

    def greet(device):
        pl.semaphore_signal(barrier, inc=1, device_id=device, device_id_type=MESH)

    for a in (2, 3, 1, 0):
        for k in (2, 1, 3, 0):
            if a or k:
                greet((tab, lax.rem(cand + a, ncand), lax.rem(dp + k, ndp)))
    for k in range(1, NZ):
        greet((lax.rem(zi + k, NZ) * NX + xi, cand, dp))
    for k in range(1, NX):
        greet((zi * NX + lax.rem(xi + k, NX), cand, dp))

    done = [0]

    def tower(chunks):
        if done[0] == 0:
            for k in range(3):
                loads[k].wait()
        first = done[0]
        done[0] += chunks

        @pl.loop(first, first + chunks)
        def _(c):
            at = pl.ds(pl.multiple_of(c * USERS_AT_ONCE, USERS_AT_ONCE), USERS_AT_ONCE)
            hidden = jnp.dot(xv[at, :], w1v[...], preferred_element_type=f32)
            hidden = (0.5 * hidden * (1.0 + lax.erf(hidden * f32(0.5**0.5)))).astype(bf16)
            users = unit_rows(jnp.dot(hidden, w2v[...], preferred_element_type=f32))
            high, low = split2((users * (logit_scale / users.shape[1])).T)
            high_ref[:, at] = high
            low_ref[:, at] = low

    square = (128, 128)
    eye = iota(square, 0) == iota(square, 1)
    for b in range(part_ref.shape[0] // 128):
        spread = jnp.broadcast_to(len_ref[:, 128 * b : 128 * (b + 1)].astype(f32), square)
        columns[128 * b : 128 * (b + 1), :] = jnp.dot(
            jnp.where(eye, spread, f32(0.0)).astype(bf16), jnp.ones(square, bf16), preferred_element_type=f32
        )

    for c in range(CHUNKS):
        table_loads[c].wait()
        if c == CHUNKS - 2:
            for load in loads:
                load.start()

        @pl.loop(0, chunk // 256)
        def _(s):
            at = pl.ds(pl.multiple_of(c * chunk + s * 256, 256), 256)
            wide[at, :] = stage[at, :].astype(f32)

    list_copy.wait()
    listed[CAPACITY:, :] = jnp.zeros_like(listed[CAPACITY:, :])
    for line in range(LINES):

        @pl.loop(0, min(128, CAPACITY - 128 * line) // TOGETHER)
        def _(g):
            at = pl.multiple_of(g * TOGETHER, TOGETHER)
            fetched = []
            for q in range(TOGETHER):
                fetched.append(wide[pl.ds(slist[line, at + q], 1), :])
            for q in range(TOGETHER):
                listed[pl.ds(line * 128 + at + q, 1), :] = fetched[q]

    pl.semaphore_wait(barrier, groups - 1 + NZ - 1 + NX - 1)
    picked = listed[...].astype(bf16)
    wanted = vlist[8:, :]
    turns = (3, 2, 1, 0)
    beside = {3: 3 - zi, 2: lax.rem(zi + 2, NZ), 1: zi + 1 - 2 * lax.rem(zi, 2), 0: zi}
    xcopies = []
    for n, k in enumerate(turns):
        zp = beside[k]
        for h in range(NX * per // 128):
            start = pl.multiple_of(zp * (NX * per) + 128 * h, 128)
            select = jnp.concatenate(
                [
                    jnp.where(wanted[line : line + 1, :] == iota(square, 0) + (start + 1), f32(1.0), f32(0.0)).astype(bf16)
                    for line in range(LINES)
                ],
                axis=1,
            )
            at = pl.ds(start, 128)
            part_ref[at, :] = (jnp.dot(select, picked, preferred_element_type=f32) + extra_ref[at, :]) / columns[at, :]
        row = []
        for o in (2, 1, 3):
            xp = lax.rem(xi + o, NX)
            copy = pltpu.make_async_remote_copy(
                src_ref=part_ref.at[pl.ds(pl.multiple_of((zp * NX + xp) * per, per), per)],
                dst_ref=recvx.at[n, o - 1],
                send_sem=sx.at[n, o - 1],
                recv_sem=rx.at[n, o - 1],
                device_id=(zi * NX + xp, cand, dp),
                device_id_type=MESH,
            )
            copy.start()
            row.append(copy)
        xcopies.append(row)

    tower(PLAN[1])

    zcopies = []
    pooled = None
    for n, k in enumerate(turns):
        zp = beside[k]
        for copy in xcopies[n]:
            copy.wait_recv()
        mine = part_ref[pl.ds(pl.multiple_of((zp * NX + xi) * per, per), per), :]
        total = mine + recvx[n, 0] + recvx[n, 1] + recvx[n, 2]
        if k == 0:
            pooled = total
        else:
            sendz[k - 1] = total
            copy = pltpu.make_async_remote_copy(
                src_ref=sendz.at[k - 1],
                dst_ref=recvz.at[k - 1],
                send_sem=sz.at[k - 1],
                recv_sem=rz.at[k - 1],
                device_id=(zp * NX + xi, cand, dp),
                device_id_type=MESH,
            )
            copy.start()
            zcopies.append(copy)
    tower(PLAN[2])
    loads[3].wait()
    for copy in zcopies:
        copy.wait_recv()
    pooled = pooled + recvz[0] + recvz[1] + recvz[2]

    p0 = pooled.astype(bf16)
    rest = pooled - p0.astype(f32)
    p1 = rest.astype(bf16)
    p2 = (rest - p1.astype(f32)).astype(bf16)
    terms = jnp.dot(jnp.concatenate([p0, p1, p2], axis=0), wv[...], preferred_element_type=f32)
    terms = terms[:per] + terms[per : 2 * per] + terms[2 * per :]
    for b in range(groups):
        sendt[b] = terms[b * own : (b + 1) * own, :]

    for a in (2, 3, 1, 0):
        for k in (2, 1, 3, 0):
            if a or k:
                there, that = lax.rem(cand + a, ncand), lax.rem(dp + k, ndp)
                pltpu.make_async_remote_copy(
                    src_ref=sendt.at[there * ndp + that],
                    dst_ref=recvt.at[a * ndp + k - 1],
                    send_sem=st,
                    recv_sem=rt,
                    device_id=(tab, there, that),
                    device_id_type=MESH,
                ).start()

    tower(PLAN[3])
    all_t = pltpu.make_async_copy(recvt, recvt, rt)
    all_t.wait()
    total = sendt[table]
    for b in range(groups - 1):
        total = total + recvt[b]
    embed = unit_rows(total)
    embed_ref[...] = embed
    item_ref[...] = embed

    me = tab * ndp + dp

    ring = 2 * NZ
    core = lax.rem(cand, 2)
    zring = lax.div(cand, 2) * NZ + zi
    for away in (2 + 4 * core, 1, ring - 1, 0):
        zq = lax.rem(zring + away, ring)
        zp = lax.rem(zq, NZ)
        share = lax.div(zq, NZ) * 2 + core
        same = isinstance(away, int) and away == 0

        @pl.loop(1 if same else 0, NX * ndp, unroll=5 if same else 4)
        def _(n):
            xp = lax.rem(xi + lax.div(n, ndp), NX)
            pltpu.make_async_remote_copy(
                src_ref=embed_ref,
                dst_ref=gathered.at[me],
                send_sem=sg,
                recv_sem=rg.at[lax.rem(lax.div(zp, 2) + lax.div(zi, 2), 2)],
                device_id=(zp * NX + xp, share, lax.rem(dp + n, ndp)),
                device_id_type=MESH,
            ).start()

    gathered[me] = embed
    tower(PLAN[4])
    lines = place_ref.shape[0]
    half = ntab * ndp // 2

    def add_scores(side, first):
        pieces = [gathered[side * half + b] for b in range(half)]
        items = jnp.concatenate(pieces, axis=0)
        item_high, item_low = split2(items)
        count = items.shape[0]
        stacked = jnp.concatenate([item_high, item_low], axis=0)

        def score(c, _):
            at = pl.ds(pl.multiple_of(c * USERS_AT_ONCE, USERS_AT_ONCE), USERS_AT_ONCE)
            both = jnp.dot(stacked, high_ref[:, at], preferred_element_type=f32)
            rest = jnp.dot(item_high, low_ref[:, at], preferred_element_type=f32)
            scores = both[:count] + both[count:] + rest
            sums = jnp.sum(jnp.exp(scores), axis=0, keepdims=True)
            for h in range(USERS_AT_ONCE // 128):
                line = c * (USERS_AT_ONCE // 128) + h
                place = place_ref[pl.ds(line, 1), :]
                block = lax.shift_right_logical(place, 4)
                apart = (lax.shift_right_logical(block, 4) - zi) & (NZ - 1)
                apart = jnp.where(apart == 3, ring - 1, jnp.where(apart == 2, 6 - 4 * core, apart))
                from_z = (zring + apart) & (ring - 1)
                here = (block & 3) == lax.shift_right_logical(from_z, 2) * 2 + core
                row = jnp.where(here, lax.div(block, ncand) * 16 + (place & 15) - side * count, -1)
                part = scores[:, h * 128 : (h + 1) * 128]
                positive = jnp.sum(
                    jnp.where(iota((count, 128), 0) == row, part, f32(0.0)), axis=0, keepdims=True
                )
                total = sums[:, h * 128 : (h + 1) * 128]
                if not first:
                    total = total + stats[pl.ds(line, 1), :]
                    positive = positive + stats[pl.ds(line + lines, 1), :]
                stats[pl.ds(line, 1), :] = total
                stats[pl.ds(line + lines, 1), :] = positive
            return 0

        lax.fori_loop(0, high_ref.shape[1] // USERS_AT_ONCE, score, 0, unroll=UNROLL)

    most = gathered.at[pl.ds(0, ntab * ndp - 1)]
    near = gathered.at[pl.ds(0, half - 1)]
    far = gathered.at[pl.ds(0, half)]
    side = lax.div(zi, 2)
    pltpu.make_async_copy(near, near, rg.at[0]).wait()
    add_scores(side, True)
    pltpu.make_async_copy(far, far, rg.at[1]).wait()
    add_scores(1 - side, False)

    scopies = []
    for o in range(1, ncand):
        copy = pltpu.make_async_remote_copy(
            src_ref=stats,
            dst_ref=others.at[o - 1],
            send_sem=ss.at[o - 1],
            recv_sem=rs.at[o - 1],
            device_id=(tab, lax.rem(cand + o, ncand), dp),
            device_id_type=MESH,
        )
        copy.start()
        scopies.append(copy)
    for row in xcopies:
        for copy in row:
            copy.wait_send()
    for copy in zcopies:
        copy.wait_send()
    pltpu.make_async_copy(recvt, recvt, st).wait()
    pltpu.make_async_copy(most, most, sg).wait()
    for copy in scopies:
        copy.wait_recv()
    both = stats[...] + others[0] + others[1] + others[2]
    loss_ref[...] = jnp.log(both[:lines]) - both[lines:]
    for copy in scopies:
        copy.wait_send()


def step(flat, extra, lengths, table, item_weight, features, user_w1, user_w2, places):
    items, width = extra.shape
    rows = table.shape[0]
    users, features_in = features.shape
    hidden, embed = user_w2.shape
    per = items // (NX * NZ)
    own = per // 16
    lines = users // 128
    vmem = pl.BlockSpec(memory_space=pltpu.VMEM)
    hbm = pl.BlockSpec(memory_space=pltpu.HBM)
    dma = pltpu.SemaphoreType.DMA
    return pl.pallas_call(
        step_kernel,
        name="step",
        out_shape=(jax.ShapeDtypeStruct((own, embed), f32), jax.ShapeDtypeStruct((lines, 128), f32)),
        in_specs=[vmem, vmem, vmem, hbm, hbm, hbm, hbm, hbm, vmem],
        out_specs=(vmem, vmem),
        scratch_shapes=[
            pltpu.VMEM((rows, width), bf16),
            pltpu.VMEM((rows, width), f32),
            pltpu.VMEM((128 * LINES, width), f32),
            pltpu.VMEM((items, width), f32),
            pltpu.VMEM((items, width), f32),
            pltpu.VMEM((users, features_in), bf16),
            pltpu.VMEM((features_in, hidden), bf16),
            pltpu.VMEM((hidden, embed), bf16),
            pltpu.VMEM((width, embed), bf16),
            pltpu.VMEM((embed, users), bf16),
            pltpu.VMEM((embed, users), bf16),
            pltpu.VMEM((NZ, NX - 1, per, width), f32),
            pltpu.VMEM((NZ - 1, per, width), f32),
            pltpu.VMEM((NZ - 1, per, width), f32),
            pltpu.VMEM((16, own, embed), f32),
            pltpu.VMEM((15, own, embed), f32),
            pltpu.VMEM((own, embed), f32),
            pltpu.VMEM((64, own, embed), f32),
            pltpu.VMEM((2 * lines, 128), f32),
            pltpu.VMEM((3, 2 * lines, 128), f32),
            pltpu.SMEM((8, 128), i32),
            dma,
            dma((CHUNKS,)),
            dma((4,)),
            dma((NZ, NX - 1)),
            dma((NZ, NX - 1)),
            dma((NZ - 1,)),
            dma((NZ - 1,)),
            dma,
            dma,
            dma,
            dma((2,)),
            dma((3,)),
            dma((3,)),
        ],
        compiler_params=pltpu.CompilerParams(
            collective_id=0, has_side_effects=True, vmem_limit_bytes=52 * 2**20
        ),
        cost_estimate=pl.CostEstimate(flops=5 * 10**9, bytes_accessed=5 * 2**20, transcendentals=0),
    )(flat, extra, lengths, table, item_weight, features, user_w1, user_w2, places)


def finish_kernel(item_ref, loss_ref, item_out, loss_out):
    item_out[...] = item_ref[...]
    loss_out[...] = loss_ref[...]


def finish(item_emb, loss):
    vmem = pl.BlockSpec(memory_space=pltpu.VMEM)
    return pl.pallas_call(
        finish_kernel,
        name="finish",
        out_shape=(
            jax.ShapeDtypeStruct(item_emb.shape, f32),
            jax.ShapeDtypeStruct(loss.shape, f32),
        ),
        in_specs=[vmem, vmem],
        out_specs=(vmem, vmem),
        compiler_params=pltpu.CompilerParams(vmem_limit_bytes=2**20),
    )(item_emb, loss)


def body(
    tables, bag_ids, bag_lengths, item_weight, user_features, user_w1, user_w2, positive_items
):
    ids = bag_ids[0].T
    ids = jnp.where(iota(ids.shape, 0) < bag_lengths, ids, i32(-1))
    flat, extra = make_list(ids, tables[0])
    item_emb, loss = step(
        flat, extra, bag_lengths, tables[0], item_weight, user_features, user_w1, user_w2, positive_items.reshape(-1, 128)
    )
    item_emb, loss = finish(item_emb, loss)
    return (item_emb, loss.reshape(-1))


def solution(mesh):
    placed = (
        P(("cand", "dp"), "tab", None),
        P(("cand", "dp"), None, None),
        P(("cand", "dp"), None),
        P(),
        P(("tab", "dp"), None),
        P(),
        P(),
        P(("tab", "dp")),
    )
    return jax.shard_map(
        body,
        mesh=mesh,
        in_specs=placed,
        out_specs=(P(("tab", "cand", "dp"), None), P(("tab", "dp"))),
        check_vma=False,
    )
```

```python
import functools
import jax
import jax.numpy as jnp
from jax import lax
from jax.experimental import pallas as pl
from jax.experimental.pallas import tpu as pltpu
from jax.sharding import PartitionSpec as P

MESH = pl.DeviceIdType.MESH
f32, bf16, i32 = jnp.float32, jnp.bfloat16, jnp.int32
epsilon = 1e-06
logit_scale = 20.0
NX, NZ = 4, 4
PARTS = 4
DEPTH = 16
CHUNKS = 8
CAPACITY = 704
LINES = 6
LANE_DEPTH = 24


def iota(shape, dim):
    return lax.broadcasted_iota(i32, shape, dim)


def list_kernel(ids_ref, table_ref, list_out, extra_ref, stage, tab, acc0, acc1, acc2, acc3,
                rank_ref, code_ref, list_ref, slist, load_sems, list_sem):
    rows = table_ref.shape[0]
    positions, items = ids_ref.shape
    tiles = items // 128
    chunk = rows // CHUNKS
    base = lax.axis_index("tab") * rows
    accs = (acc0, acc1, acc2, acc3)

    slots = tiles * positions
    ids = jnp.concatenate([ids_ref[:, 128 * t : 128 * (t + 1)] for t in range(tiles)], axis=0)
    r = iota((slots, 128), 0)
    lane = iota((slots, 128), 1)
    local = ids - base
    live = (local >= 0) & (local < rows)
    item = lax.div(r, positions) * 128 + lane
    code = local * 2048 + item + 1
    below = jnp.where(iota((slots, slots), 0) >= iota((slots, slots), 1), f32(1.0), f32(0.0)).astype(bf16)
    ones = jnp.ones((128, 128), bf16)

    def ordered(which):
        marks = jnp.where(which, f32(1.0), f32(0.0)).astype(bf16)
        order = jnp.dot(below, marks, preferred_element_type=f32)
        return order, jnp.where(which, order - 1.0, f32(-1.0)).astype(i32)

    order, rank = ordered(live)
    counts = jnp.minimum(order[slots - 1 : slots, :], f32(LANE_DEPTH))
    square = (128, 128)
    before = iota(square, 0) < iota(square, 1)
    offset = jnp.dot(
        jnp.broadcast_to(counts, (8, 128)).astype(bf16),
        jnp.where(before, f32(1.0), f32(0.0)).astype(bf16),
        preferred_element_type=f32,
    )
    spread = jnp.broadcast_to(counts, square)
    after = iota(square, 0) > iota(square, 1)
    eye = iota(square, 0) == iota(square, 1)
    column = jnp.dot(
        jnp.concatenate([jnp.where(after, spread, f32(0.0)), jnp.where(eye, spread, f32(0.0))], axis=0).astype(bf16),
        ones,
        preferred_element_type=f32,
    )
    offset_column, count_column = column[:128].astype(i32), column[128:].astype(i32)
    offset_row = offset[:1].astype(i32)
    lane_square = iota(square, 1)
    lines = iota((8, 128), 0)
    left, right = [], []
    for k in range(LANE_DEPTH):
        found = jnp.sum(jnp.where(rank == k, code, 0), axis=0, keepdims=True)
        where_to = jnp.broadcast_to(lax.shift_right_logical(offset_row + k, 7), (8, 128)) == lines
        left.append(
            jnp.concatenate(
                [
                    jnp.where(where_to, jnp.broadcast_to(lax.shift_right_logical(found, 7 * p) & 127, (8, 128)), 0)
                    for p in range(4)
                ],
                axis=0,
            ).astype(f32).astype(bf16)
        )
        hit = (((offset_column + k) & 127) == lane_square) & (count_column > k)
        right.append(jnp.where(hit, f32(1.0), f32(0.0)).astype(bf16))
    flat = jnp.dot(
        jnp.concatenate(left, axis=1), jnp.concatenate(right, axis=0), preferred_element_type=f32
    ).astype(i32)
    codes = flat[:8] + flat[8:16] * 128 + flat[16:24] * 16384 + flat[24:32] * 2097152
    list_out[:8, :] = lax.shift_right_logical(codes, 11)
    list_out[8:, :] = codes & 2047
    extra_ref[...] = jnp.zeros_like(extra_ref)

    place = offset_row + rank
    over = live & ((rank >= LANE_DEPTH) | (place >= CAPACITY))
    beyond = jnp.max(jnp.where(over, f32(1.0), f32(0.0)))

    @pl.when(beyond > 0.0)
    def _():
        loads = [
            pltpu.make_async_copy(
                table_ref.at[pl.ds(c * chunk, chunk)], stage.at[pl.ds(c * chunk, chunk)], load_sems.at[c]
            )
            for c in range(CHUNKS)
        ]
        for load in loads:
            load.start()
        order, rank = ordered(over)
        rank_ref[...] = rank
        code_ref[...] = code
        counts = order[slots - 1 : slots, :].astype(i32)
        most = jnp.max(counts)
        for acc in accs:
            acc[...] = jnp.zeros_like(acc)
        for load in loads:
            load.wait()

        @pl.loop(0, rows // 256)
        def _(s):
            at = pl.ds(pl.multiple_of(s * 256, 256), 256)
            tab[at, :] = stage[at, :].astype(f32)

        def more(b, _):
            for k in range(DEPTH):
                found = jnp.sum(
                    jnp.where(rank_ref[...] == b * DEPTH + k, code_ref[...], 0), axis=0, keepdims=True
                )
                list_ref[k : k + 1, :] = found
            list_ref[DEPTH : DEPTH + 1, :] = jnp.clip(counts - b * DEPTH, 0, DEPTH)
            copy = pltpu.make_async_copy(list_ref, slist, list_sem)
            copy.start()
            copy.wait()

            @pl.loop(0, 128)
            def _(at):
                def group(g, _):
                    for q in range(PARTS):
                        code = slist[g * PARTS + q, at]
                        row = lax.shift_right_logical(code, 11)
                        to = code & 2047
                        accs[q][pl.ds(to, 1), :] += tab[pl.ds(row, 1), :]
                    return 0

                lax.fori_loop(0, lax.shift_right_logical(slist[DEPTH, at] + PARTS - 1, 2), group, 0)

            return 0

        lax.fori_loop(0, lax.div(most + DEPTH - 1, DEPTH), more, 0)
        extra_ref[...] = acc0[1 : items + 1, :] + acc1[1 : items + 1, :] + acc2[1 : items + 1, :] + acc3[1 : items + 1, :]


def make_list(ids_t, table):
    rows, width = table.shape
    positions, items = ids_t.shape
    slots = positions * items // 128
    vmem = pl.BlockSpec(memory_space=pltpu.VMEM)
    return pl.pallas_call(
        list_kernel,
        name="list",
        out_shape=(jax.ShapeDtypeStruct((16, 128), i32), jax.ShapeDtypeStruct((items, width), f32)),
        in_specs=[vmem, pl.BlockSpec(memory_space=pltpu.HBM)],
        out_specs=(vmem, vmem),
        scratch_shapes=[
            pltpu.VMEM((rows, width), bf16),
            pltpu.VMEM((rows, width), f32),
            *[pltpu.VMEM((items + 8, width), f32)] * PARTS,
            pltpu.VMEM((slots, 128), i32),
            pltpu.VMEM((slots, 128), i32),
            pltpu.VMEM((DEPTH + 8, 128), i32),
            pltpu.SMEM((DEPTH + 8, 128), i32),
            pltpu.SemaphoreType.DMA((CHUNKS,)),
            pltpu.SemaphoreType.DMA,
        ],
        compiler_params=pltpu.CompilerParams(vmem_limit_bytes=52 * 2**20),
        cost_estimate=pl.CostEstimate(flops=10**8, bytes_accessed=2**20, transcendentals=0),
    )(ids_t, table)


def split2(v):
    high = v.astype(bf16)
    return high, (v - high.astype(f32)).astype(bf16)


def unit_rows(v):
    return v * lax.rsqrt(jnp.mean(v * v, axis=-1, keepdims=True) + epsilon)


PLAN = (0, 3, 1, 1, 3)
USERS_AT_ONCE = 256
TOGETHER = 16
UNROLL = 4


def step_kernel(vlist, extra_ref, len_ref, table_ref, weight_ref, x_ref, w1_ref, w2_ref, place_ref, item_ref, loss_ref,
                stage, wide, listed, part_ref, columns, xv, w1v, w2v, wv, high_ref, low_ref, recvx, sendz, recvz, sendt, recvt, embed_ref,
                gathered, stats, others, slist, list_sem, table_sems, load_sems, sx, rx, sz, rz, st, rt, sg, rg, ss, rs):
    tab, cand, dp = lax.axis_index("tab"), lax.axis_index("cand"), lax.axis_index("dp")
    xi, zi = lax.rem(tab, NX), lax.div(tab, NX)
    ntab, ncand, ndp = NX * NZ, 4, 4
    width = part_ref.shape[1]
    per = part_ref.shape[0] // ntab
    groups = ncand * ndp
    own = per // groups
    table = cand * ndp + dp

    list_copy = pltpu.make_async_copy(vlist.at[pl.ds(0, 8)], slist, list_sem)
    list_copy.start()

    def local(src, dst, k):
        return pltpu.make_async_copy(src, dst, load_sems.at[k])

    rows = table_ref.shape[0]
    chunk = rows // CHUNKS
    table_loads = []
    for c in range(CHUNKS):
        at = pl.ds(c * chunk, chunk)
        table_loads.append(pltpu.make_async_copy(table_ref.at[at], stage.at[at], table_sems.at[c]))
        table_loads[-1].start()

    loads = [
        local(x_ref, xv, 0),
        local(w1_ref, w1v, 1),
        local(w2_ref, w2v, 2),
        local(weight_ref.at[pl.ds(pl.multiple_of(table * width, width), width)], wv, 3),
    ]

    barrier = pltpu.get_barrier_semaphore()

    def greet(device):
        pl.semaphore_signal(barrier, inc=1, device_id=device, device_id_type=MESH)

    ring = 2 * NZ
    core = lax.rem(cand, 2)
    zring = lax.div(cand, 2) * NZ + zi
    opposite = lax.rem(zi + 2, NZ) * NX + xi
    for k in (2, 1, 3, 0):
        for a in range(ncand):
            greet((opposite, a, lax.rem(dp + k, ndp)))
    for k in (1, 3):
        greet((lax.rem(zi + k, NZ) * NX + xi, cand, dp))
    for k in range(1, NX):
        greet((zi * NX + lax.rem(xi + k, NX), cand, dp))

    done = [0]

    def tower(chunks):
        if done[0] == 0:
            for k in range(3):
                loads[k].wait()
        first = done[0]
        done[0] += chunks

        @pl.loop(first, first + chunks)
        def _(c):
            at = pl.ds(pl.multiple_of(c * USERS_AT_ONCE, USERS_AT_ONCE), USERS_AT_ONCE)
            hidden = jnp.dot(xv[at, :], w1v[...], preferred_element_type=f32)
            hidden = (0.5 * hidden * (1.0 + lax.erf(hidden * f32(0.5**0.5)))).astype(bf16)
            users = unit_rows(jnp.dot(hidden, w2v[...], preferred_element_type=f32))
            high, low = split2((users * (logit_scale / users.shape[1])).T)
            high_ref[:, at] = high
            low_ref[:, at] = low

    square = (128, 128)
    eye = iota(square, 0) == iota(square, 1)
    for b in range(part_ref.shape[0] // 128):
        spread = jnp.broadcast_to(len_ref[:, 128 * b : 128 * (b + 1)].astype(f32), square)
        columns[128 * b : 128 * (b + 1), :] = jnp.dot(
            jnp.where(eye, spread, f32(0.0)).astype(bf16), jnp.ones(square, bf16), preferred_element_type=f32
        )

    for c in range(CHUNKS):
        table_loads[c].wait()
        if c == CHUNKS - 2:
            for load in loads:
                load.start()

        @pl.loop(0, chunk // 256)
        def _(s):
            at = pl.ds(pl.multiple_of(c * chunk + s * 256, 256), 256)
            wide[at, :] = stage[at, :].astype(f32)

    list_copy.wait()
    listed[CAPACITY:, :] = jnp.zeros_like(listed[CAPACITY:, :])
    for line in range(LINES):

        @pl.loop(0, min(128, CAPACITY - 128 * line) // TOGETHER)
        def _(g):
            at = pl.multiple_of(g * TOGETHER, TOGETHER)
            fetched = []
            for q in range(TOGETHER):
                fetched.append(wide[pl.ds(slist[line, at + q], 1), :])
            for q in range(TOGETHER):
                listed[pl.ds(line * 128 + at + q, 1), :] = fetched[q]

    pl.semaphore_wait(barrier, groups + NZ - 2 + NX - 1)
    picked = listed[...].astype(bf16)
    wanted = vlist[8:, :]
    turns = (3, 2, 1, 0)
    beside = {3: 3 - zi, 2: lax.rem(zi + 2, NZ), 1: zi + 1 - 2 * lax.rem(zi, 2), 0: zi}
    xcopies = []
    for n, k in enumerate(turns):
        zp = beside[k]
        for h in range(NX * per // 128):
            start = pl.multiple_of(zp * (NX * per) + 128 * h, 128)
            select = jnp.concatenate(
                [
                    jnp.where(wanted[line : line + 1, :] == iota(square, 0) + (start + 1), f32(1.0), f32(0.0)).astype(bf16)
                    for line in range(LINES)
                ],
                axis=1,
            )
            at = pl.ds(start, 128)
            part_ref[at, :] = (jnp.dot(select, picked, preferred_element_type=f32) + extra_ref[at, :]) / columns[at, :]
        row = []
        for o in (2, 1, 3):
            xp = lax.rem(xi + o, NX)
            copy = pltpu.make_async_remote_copy(
                src_ref=part_ref.at[pl.ds(pl.multiple_of((zp * NX + xp) * per, per), per)],
                dst_ref=recvx.at[n, o - 1],
                send_sem=sx.at[n, o - 1],
                recv_sem=rx.at[n, o - 1],
                device_id=(zi * NX + xp, cand, dp),
                device_id_type=MESH,
            )
            copy.start()
            row.append(copy)
        xcopies.append(row)

    tower(PLAN[1])

    zcopies = []
    pooled = None
    for n, k in enumerate(turns):
        zp = beside[k]
        for copy in xcopies[n]:
            copy.wait_recv()
        mine = part_ref[pl.ds(pl.multiple_of((zp * NX + xi) * per, per), per), :]
        total = mine + recvx[n, 0] + recvx[n, 1] + recvx[n, 2]
        if k == 0:
            pooled = total
        else:
            sendz[k - 1] = total
            copy = pltpu.make_async_remote_copy(
                src_ref=sendz.at[k - 1],
                dst_ref=recvz.at[k - 1],
                send_sem=sz.at[k - 1],
                recv_sem=rz.at[k - 1],
                device_id=(zp * NX + xi, cand, dp),
                device_id_type=MESH,
            )
            copy.start()
            zcopies.append(copy)
    tower(PLAN[2])
    loads[3].wait()
    for copy in zcopies:
        copy.wait_recv()
    pooled = pooled + recvz[0] + recvz[1] + recvz[2]

    p0 = pooled.astype(bf16)
    rest = pooled - p0.astype(f32)
    p1 = rest.astype(bf16)
    p2 = (rest - p1.astype(f32)).astype(bf16)
    terms = jnp.dot(jnp.concatenate([p0, p1, p2], axis=0), wv[...], preferred_element_type=f32)
    terms = terms[:per] + terms[per : 2 * per] + terms[2 * per :]
    for b in range(groups):
        sendt[b] = terms[b * own : (b + 1) * own, :]

    for k in (2, 1, 3, 0):
        for a in range(ncand):
            that = lax.rem(dp + k, ndp)
            holder = lax.rem((a // 2) * NZ + zi + (2 if a % 2 else ring - 2), ring)
            pltpu.make_async_remote_copy(
                src_ref=sendt.at[a * ndp + that],
                dst_ref=recvt.at[table],
                send_sem=st,
                recv_sem=rt,
                device_id=(opposite, lax.div(holder, NZ) * 2 + a % 2, that),
                device_id_type=MESH,
            ).start()

    tower(PLAN[3])
    all_t = pltpu.make_async_copy(recvt, recvt, rt)
    all_t.wait()
    total = recvt[0]
    for b in range(1, groups):
        total = total + recvt[b]
    embed = unit_rows(total)
    embed_ref[...] = embed

    me = tab * ndp + dp

    for away in (2 + 4 * core, 1, ring - 1, 0):
        zq = lax.rem(zring + away, ring)
        zp = lax.rem(zq, NZ)
        share = lax.div(zq, NZ) * 2 + core
        same = isinstance(away, int) and away == 0

        @pl.loop(1 if same else 0, NX * ndp, unroll=5 if same else 4)
        def _(n):
            xp = lax.rem(xi + lax.div(n, ndp), NX)
            pltpu.make_async_remote_copy(
                src_ref=embed_ref,
                dst_ref=gathered.at[me],
                send_sem=sg,
                recv_sem=rg.at[lax.rem(lax.div(zp, 2) + lax.div(zi, 2), 2)],
                device_id=(zp * NX + xp, share, lax.rem(dp + n, ndp)),
                device_id_type=MESH,
            ).start()

    gathered[me] = embed
    tower(PLAN[4])
    lines = place_ref.shape[0]
    half = ntab * ndp // 2

    def add_scores(side, first):
        pieces = [gathered[side * half + b] for b in range(half)]
        items = jnp.concatenate(pieces, axis=0)
        item_high, item_low = split2(items)
        count = items.shape[0]
        stacked = jnp.concatenate([item_high, item_low], axis=0)

        def score(c, _):
            at = pl.ds(pl.multiple_of(c * USERS_AT_ONCE, USERS_AT_ONCE), USERS_AT_ONCE)
            both = jnp.dot(stacked, high_ref[:, at], preferred_element_type=f32)
            rest = jnp.dot(item_high, low_ref[:, at], preferred_element_type=f32)
            scores = both[:count] + both[count:] + rest
            sums = jnp.sum(jnp.exp(scores), axis=0, keepdims=True)
            for h in range(USERS_AT_ONCE // 128):
                line = c * (USERS_AT_ONCE // 128) + h
                place = place_ref[pl.ds(line, 1), :]
                block = lax.shift_right_logical(place, 4)
                apart = (lax.shift_right_logical(block, 4) + 2 - zi) & (NZ - 1)
                apart = jnp.where(apart == 3, ring - 1, jnp.where(apart == 2, 6 - 4 * core, apart))
                owner = (zring + apart + 2 + 4 * core) & (ring - 1)
                here = (block & 3) == lax.shift_right_logical(owner, 2) * 2 + core
                slot = (lax.shift_right_logical(block, 2) + 2 * NX) & (ntab - 1)
                row = jnp.where(here, slot * 16 + (place & 15) - side * count, -1)
                part = scores[:, h * 128 : (h + 1) * 128]
                positive = jnp.sum(
                    jnp.where(iota((count, 128), 0) == row, part, f32(0.0)), axis=0, keepdims=True
                )
                total = sums[:, h * 128 : (h + 1) * 128]
                if not first:
                    total = total + stats[pl.ds(line, 1), :]
                    positive = positive + stats[pl.ds(line + lines, 1), :]
                stats[pl.ds(line, 1), :] = total
                stats[pl.ds(line + lines, 1), :] = positive
            return 0

        lax.fori_loop(0, high_ref.shape[1] // USERS_AT_ONCE, score, 0, unroll=UNROLL)

    most = gathered.at[pl.ds(0, ntab * ndp - 1)]
    near = gathered.at[pl.ds(0, half - 1)]
    far = gathered.at[pl.ds(0, half)]
    side = lax.div(zi, 2)
    pltpu.make_async_copy(near, near, rg.at[0]).wait()
    add_scores(side, True)
    pltpu.make_async_copy(far, far, rg.at[1]).wait()
    item_ref[...] = gathered[opposite * ndp + dp]
    add_scores(1 - side, False)

    scopies = []
    for o in range(1, ncand):
        copy = pltpu.make_async_remote_copy(
            src_ref=stats,
            dst_ref=others.at[o - 1],
            send_sem=ss.at[o - 1],
            recv_sem=rs.at[o - 1],
            device_id=(tab, lax.rem(cand + o, ncand), dp),
            device_id_type=MESH,
        )
        copy.start()
        scopies.append(copy)
    for row in xcopies:
        for copy in row:
            copy.wait_send()
    for copy in zcopies:
        copy.wait_send()
    pltpu.make_async_copy(recvt, recvt, st).wait()
    pltpu.make_async_copy(most, most, sg).wait()
    for copy in scopies:
        copy.wait_recv()
    both = stats[...] + others[0] + others[1] + others[2]
    loss_ref[...] = jnp.log(both[:lines]) - both[lines:]
    for copy in scopies:
        copy.wait_send()


def step(flat, extra, lengths, table, item_weight, features, user_w1, user_w2, places):
    items, width = extra.shape
    rows = table.shape[0]
    users, features_in = features.shape
    hidden, embed = user_w2.shape
    per = items // (NX * NZ)
    own = per // 16
    lines = users // 128
    vmem = pl.BlockSpec(memory_space=pltpu.VMEM)
    hbm = pl.BlockSpec(memory_space=pltpu.HBM)
    dma = pltpu.SemaphoreType.DMA
    return pl.pallas_call(
        step_kernel,
        name="step",
        out_shape=(jax.ShapeDtypeStruct((own, embed), f32), jax.ShapeDtypeStruct((lines, 128), f32)),
        in_specs=[vmem, vmem, vmem, hbm, hbm, hbm, hbm, hbm, vmem],
        out_specs=(vmem, vmem),
        scratch_shapes=[
            pltpu.VMEM((rows, width), bf16),
            pltpu.VMEM((rows, width), f32),
            pltpu.VMEM((128 * LINES, width), f32),
            pltpu.VMEM((items, width), f32),
            pltpu.VMEM((items, width), f32),
            pltpu.VMEM((users, features_in), bf16),
            pltpu.VMEM((features_in, hidden), bf16),
            pltpu.VMEM((hidden, embed), bf16),
            pltpu.VMEM((width, embed), bf16),
            pltpu.VMEM((embed, users), bf16),
            pltpu.VMEM((embed, users), bf16),
            pltpu.VMEM((NZ, NX - 1, per, width), f32),
            pltpu.VMEM((NZ - 1, per, width), f32),
            pltpu.VMEM((NZ - 1, per, width), f32),
            pltpu.VMEM((16, own, embed), f32),
            pltpu.VMEM((16, own, embed), f32),
            pltpu.VMEM((own, embed), f32),
            pltpu.VMEM((64, own, embed), f32),
            pltpu.VMEM((2 * lines, 128), f32),
            pltpu.VMEM((3, 2 * lines, 128), f32),
            pltpu.SMEM((8, 128), i32),
            dma,
            dma((CHUNKS,)),
            dma((4,)),
            dma((NZ, NX - 1)),
            dma((NZ, NX - 1)),
            dma((NZ - 1,)),
            dma((NZ - 1,)),
            dma,
            dma,
            dma,
            dma((2,)),
            dma((3,)),
            dma((3,)),
        ],
        compiler_params=pltpu.CompilerParams(
            collective_id=0, has_side_effects=True, vmem_limit_bytes=52 * 2**20
        ),
        cost_estimate=pl.CostEstimate(flops=5 * 10**9, bytes_accessed=5 * 2**20, transcendentals=0),
    )(flat, extra, lengths, table, item_weight, features, user_w1, user_w2, places)


def finish_kernel(item_ref, loss_ref, item_out, loss_out):
    item_out[...] = item_ref[...]
    loss_out[...] = loss_ref[...]


def finish(item_emb, loss):
    vmem = pl.BlockSpec(memory_space=pltpu.VMEM)
    return pl.pallas_call(
        finish_kernel,
        name="finish",
        out_shape=(
            jax.ShapeDtypeStruct(item_emb.shape, f32),
            jax.ShapeDtypeStruct(loss.shape, f32),
        ),
        in_specs=[vmem, vmem],
        out_specs=(vmem, vmem),
        compiler_params=pltpu.CompilerParams(vmem_limit_bytes=2**20),
    )(item_emb, loss)


def body(
    tables, bag_ids, bag_lengths, item_weight, user_features, user_w1, user_w2, positive_items
):
    ids = bag_ids[0].T
    ids = jnp.where(iota(ids.shape, 0) < bag_lengths, ids, i32(-1))
    flat, extra = make_list(ids, tables[0])
    item_emb, loss = step(
        flat, extra, bag_lengths, tables[0], item_weight, user_features, user_w1, user_w2, positive_items.reshape(-1, 128)
    )
    item_emb, loss = finish(item_emb, loss)
    return (item_emb, loss.reshape(-1))


def solution(mesh):
    placed = (
        P(("cand", "dp"), "tab", None),
        P(("cand", "dp"), None, None),
        P(("cand", "dp"), None),
        P(),
        P(("tab", "dp"), None),
        P(),
        P(),
        P(("tab", "dp")),
    )
    return jax.shard_map(
        body,
        mesh=mesh,
        in_specs=placed,
        out_specs=(P(("tab", "cand", "dp"), None), P(("tab", "dp"))),
        check_vma=False,
    )
```

```python
import functools
import jax
import jax.numpy as jnp
from jax import lax
from jax.experimental import pallas as pl
from jax.experimental.pallas import tpu as pltpu
from jax.sharding import PartitionSpec as P

MESH = pl.DeviceIdType.MESH
f32, bf16, i32 = jnp.float32, jnp.bfloat16, jnp.int32
epsilon = 1e-06
logit_scale = 20.0
NX, NZ = 4, 4
PARTS = 4
DEPTH = 16
CHUNKS = 8
CAPACITY = 704
LINES = 6
LANE_DEPTH = 24


def iota(shape, dim):
    return lax.broadcasted_iota(i32, shape, dim)


def list_kernel(ids_ref, table_ref, list_out, extra_ref, stage, tab, acc0, acc1, acc2, acc3,
                rank_ref, code_ref, list_ref, slist, load_sems, list_sem):
    rows = table_ref.shape[0]
    positions, items = ids_ref.shape
    tiles = items // 128
    chunk = rows // CHUNKS
    base = lax.axis_index("tab") * rows
    accs = (acc0, acc1, acc2, acc3)

    slots = tiles * positions
    ids = jnp.concatenate([ids_ref[:, 128 * t : 128 * (t + 1)] for t in range(tiles)], axis=0)
    r = iota((slots, 128), 0)
    lane = iota((slots, 128), 1)
    local = ids - base
    live = (local >= 0) & (local < rows)
    item = lax.div(r, positions) * 128 + lane
    code = local * 2048 + item + 1
    below = jnp.where(iota((slots, slots), 0) >= iota((slots, slots), 1), f32(1.0), f32(0.0)).astype(bf16)
    ones = jnp.ones((128, 128), bf16)

    def ordered(which):
        marks = jnp.where(which, f32(1.0), f32(0.0)).astype(bf16)
        order = jnp.dot(below, marks, preferred_element_type=f32)
        return order, jnp.where(which, order - 1.0, f32(-1.0)).astype(i32)

    order, rank = ordered(live)
    counts = jnp.minimum(order[slots - 1 : slots, :], f32(LANE_DEPTH))
    square = (128, 128)
    before = iota(square, 0) < iota(square, 1)
    offset = jnp.dot(
        jnp.broadcast_to(counts, (8, 128)).astype(bf16),
        jnp.where(before, f32(1.0), f32(0.0)).astype(bf16),
        preferred_element_type=f32,
    )
    spread = jnp.broadcast_to(counts, square)
    after = iota(square, 0) > iota(square, 1)
    eye = iota(square, 0) == iota(square, 1)
    column = jnp.dot(
        jnp.concatenate([jnp.where(after, spread, f32(0.0)), jnp.where(eye, spread, f32(0.0))], axis=0).astype(bf16),
        ones,
        preferred_element_type=f32,
    )
    offset_column, count_column = column[:128].astype(i32), column[128:].astype(i32)
    offset_row = offset[:1].astype(i32)
    lane_square = iota(square, 1)
    lines = iota((8, 128), 0)
    left, right = [], []
    for k in range(LANE_DEPTH):
        found = jnp.sum(jnp.where(rank == k, code, 0), axis=0, keepdims=True)
        where_to = jnp.broadcast_to(lax.shift_right_logical(offset_row + k, 7), (8, 128)) == lines
        left.append(
            jnp.concatenate(
                [
                    jnp.where(where_to, jnp.broadcast_to(lax.shift_right_logical(found, 7 * p) & 127, (8, 128)), 0)
                    for p in range(4)
                ],
                axis=0,
            ).astype(f32).astype(bf16)
        )
        hit = (((offset_column + k) & 127) == lane_square) & (count_column > k)
        right.append(jnp.where(hit, f32(1.0), f32(0.0)).astype(bf16))
    flat = jnp.dot(
        jnp.concatenate(left, axis=1), jnp.concatenate(right, axis=0), preferred_element_type=f32
    ).astype(i32)
    codes = flat[:8] + flat[8:16] * 128 + flat[16:24] * 16384 + flat[24:32] * 2097152
    list_out[:8, :] = lax.shift_right_logical(codes, 11)
    list_out[8:, :] = codes & 2047
    extra_ref[...] = jnp.zeros_like(extra_ref)

    place = offset_row + rank
    over = live & ((rank >= LANE_DEPTH) | (place >= CAPACITY))
    beyond = jnp.max(jnp.where(over, f32(1.0), f32(0.0)))

    @pl.when(beyond > 0.0)
    def _():
        loads = [
            pltpu.make_async_copy(
                table_ref.at[pl.ds(c * chunk, chunk)], stage.at[pl.ds(c * chunk, chunk)], load_sems.at[c]
            )
            for c in range(CHUNKS)
        ]
        for load in loads:
            load.start()
        order, rank = ordered(over)
        rank_ref[...] = rank
        code_ref[...] = code
        counts = order[slots - 1 : slots, :].astype(i32)
        most = jnp.max(counts)
        for acc in accs:
            acc[...] = jnp.zeros_like(acc)
        for load in loads:
            load.wait()

        @pl.loop(0, rows // 256)
        def _(s):
            at = pl.ds(pl.multiple_of(s * 256, 256), 256)
            tab[at, :] = stage[at, :].astype(f32)

        def more(b, _):
            for k in range(DEPTH):
                found = jnp.sum(
                    jnp.where(rank_ref[...] == b * DEPTH + k, code_ref[...], 0), axis=0, keepdims=True
                )
                list_ref[k : k + 1, :] = found
            list_ref[DEPTH : DEPTH + 1, :] = jnp.clip(counts - b * DEPTH, 0, DEPTH)
            copy = pltpu.make_async_copy(list_ref, slist, list_sem)
            copy.start()
            copy.wait()

            @pl.loop(0, 128)
            def _(at):
                def group(g, _):
                    for q in range(PARTS):
                        code = slist[g * PARTS + q, at]
                        row = lax.shift_right_logical(code, 11)
                        to = code & 2047
                        accs[q][pl.ds(to, 1), :] += tab[pl.ds(row, 1), :]
                    return 0

                lax.fori_loop(0, lax.shift_right_logical(slist[DEPTH, at] + PARTS - 1, 2), group, 0)

            return 0

        lax.fori_loop(0, lax.div(most + DEPTH - 1, DEPTH), more, 0)
        extra_ref[...] = acc0[1 : items + 1, :] + acc1[1 : items + 1, :] + acc2[1 : items + 1, :] + acc3[1 : items + 1, :]


def make_list(ids_t, table):
    rows, width = table.shape
    positions, items = ids_t.shape
    slots = positions * items // 128
    vmem = pl.BlockSpec(memory_space=pltpu.VMEM)
    return pl.pallas_call(
        list_kernel,
        name="list",
        out_shape=(jax.ShapeDtypeStruct((16, 128), i32), jax.ShapeDtypeStruct((items, width), f32)),
        in_specs=[vmem, pl.BlockSpec(memory_space=pltpu.HBM)],
        out_specs=(vmem, vmem),
        scratch_shapes=[
            pltpu.VMEM((rows, width), bf16),
            pltpu.VMEM((rows, width), f32),
            *[pltpu.VMEM((items + 8, width), f32)] * PARTS,
            pltpu.VMEM((slots, 128), i32),
            pltpu.VMEM((slots, 128), i32),
            pltpu.VMEM((DEPTH + 8, 128), i32),
            pltpu.SMEM((DEPTH + 8, 128), i32),
            pltpu.SemaphoreType.DMA((CHUNKS,)),
            pltpu.SemaphoreType.DMA,
        ],
        compiler_params=pltpu.CompilerParams(vmem_limit_bytes=52 * 2**20),
        cost_estimate=pl.CostEstimate(flops=10**8, bytes_accessed=2**20, transcendentals=0),
    )(ids_t, table)


def split2(v):
    high = v.astype(bf16)
    return high, (v - high.astype(f32)).astype(bf16)


def unit_rows(v):
    return v * lax.rsqrt(jnp.mean(v * v, axis=-1, keepdims=True) + epsilon)


PLAN = (0, 3, 0, 2, 3)
USERS_AT_ONCE = 256
TOGETHER = 16
UNROLL = 4


def step_kernel(vlist, extra_ref, len_ref, table_ref, weight_ref, x_ref, w1_ref, w2_ref, place_ref, item_ref, loss_ref,
                stage, wide, listed, part_ref, columns, xv, w1v, w2v, wv, high_ref, low_ref, recvx, sendz, recvz, sendt, recvt, embed_ref,
                gathered, stats, others, slist, list_sem, table_sems, load_sems, sx, rx, sz, rz, st, rt, sg, rg, ss, rs):
    tab, cand, dp = lax.axis_index("tab"), lax.axis_index("cand"), lax.axis_index("dp")
    xi, zi = lax.rem(tab, NX), lax.div(tab, NX)
    ntab, ncand, ndp = NX * NZ, 4, 4
    width = part_ref.shape[1]
    per = part_ref.shape[0] // ntab
    groups = ncand * ndp
    own = per // groups
    table = cand * ndp + dp

    list_copy = pltpu.make_async_copy(vlist.at[pl.ds(0, 8)], slist, list_sem)
    list_copy.start()

    def local(src, dst, k):
        return pltpu.make_async_copy(src, dst, load_sems.at[k])

    rows = table_ref.shape[0]
    chunk = rows // CHUNKS
    table_loads = []
    for c in range(CHUNKS):
        at = pl.ds(c * chunk, chunk)
        table_loads.append(pltpu.make_async_copy(table_ref.at[at], stage.at[at], table_sems.at[c]))
        table_loads[-1].start()

    loads = [
        local(x_ref, xv, 0),
        local(w1_ref, w1v, 1),
        local(w2_ref, w2v, 2),
        local(weight_ref.at[pl.ds(pl.multiple_of(table * width, width), width)], wv, 3),
    ]

    barrier = pltpu.get_barrier_semaphore()

    def greet(device):
        pl.semaphore_signal(barrier, inc=1, device_id=device, device_id_type=MESH)

    ring = 2 * NZ
    core = lax.rem(cand, 2)
    zring = lax.div(cand, 2) * NZ + zi
    opposite = lax.rem(zi + 2, NZ) * NX + xi
    for k in (2, 1, 3, 0):
        for a in range(ncand):
            greet((opposite, a, lax.rem(dp + k, ndp)))
    for k in (1, 3):
        greet((lax.rem(zi + k, NZ) * NX + xi, cand, dp))
    for k in range(1, NX):
        greet((zi * NX + lax.rem(xi + k, NX), cand, dp))

    done = [0]

    def tower(chunks):
        if done[0] == 0:
            for k in range(3):
                loads[k].wait()
        first = done[0]
        done[0] += chunks

        @pl.loop(first, first + chunks)
        def _(c):
            at = pl.ds(pl.multiple_of(c * USERS_AT_ONCE, USERS_AT_ONCE), USERS_AT_ONCE)
            hidden = jnp.dot(xv[at, :], w1v[...], preferred_element_type=f32)
            hidden = (0.5 * hidden * (1.0 + lax.erf(hidden * f32(0.5**0.5)))).astype(bf16)
            users = unit_rows(jnp.dot(hidden, w2v[...], preferred_element_type=f32))
            high, low = split2((users * (logit_scale / users.shape[1])).T)
            high_ref[:, at] = high
            low_ref[:, at] = low

    square = (128, 128)
    eye = iota(square, 0) == iota(square, 1)
    for b in range(part_ref.shape[0] // 128):
        spread = jnp.broadcast_to(len_ref[:, 128 * b : 128 * (b + 1)].astype(f32), square)
        columns[128 * b : 128 * (b + 1), :] = jnp.dot(
            jnp.where(eye, spread, f32(0.0)).astype(bf16), jnp.ones(square, bf16), preferred_element_type=f32
        )

    for c in range(CHUNKS):
        table_loads[c].wait()
        if c == CHUNKS - 2:
            for load in loads:
                load.start()

        @pl.loop(0, chunk // 256)
        def _(s):
            at = pl.ds(pl.multiple_of(c * chunk + s * 256, 256), 256)
            wide[at, :] = stage[at, :].astype(f32)

    list_copy.wait()
    listed[CAPACITY:, :] = jnp.zeros_like(listed[CAPACITY:, :])
    for line in range(LINES):

        @pl.loop(0, min(128, CAPACITY - 128 * line) // TOGETHER)
        def _(g):
            at = pl.multiple_of(g * TOGETHER, TOGETHER)
            fetched = []
            for q in range(TOGETHER):
                fetched.append(wide[pl.ds(slist[line, at + q], 1), :])
            for q in range(TOGETHER):
                listed[pl.ds(line * 128 + at + q, 1), :] = fetched[q]

    pl.semaphore_wait(barrier, groups + NZ - 2 + NX - 1)
    picked = listed[...].astype(bf16)
    wanted = vlist[8:, :]
    turns = (3, 2, 1, 0)
    beside = {3: 3 - zi, 2: lax.rem(zi + 2, NZ), 1: zi + 1 - 2 * lax.rem(zi, 2), 0: zi}
    xcopies = []
    for n, k in enumerate(turns):
        zp = beside[k]
        for h in range(NX * per // 128):
            start = pl.multiple_of(zp * (NX * per) + 128 * h, 128)
            select = jnp.concatenate(
                [
                    jnp.where(wanted[line : line + 1, :] == iota(square, 0) + (start + 1), f32(1.0), f32(0.0)).astype(bf16)
                    for line in range(LINES)
                ],
                axis=1,
            )
            at = pl.ds(start, 128)
            part_ref[at, :] = (jnp.dot(select, picked, preferred_element_type=f32) + extra_ref[at, :]) / columns[at, :]
        row = []
        for o in (2, 1, 3):
            xp = lax.rem(xi + o, NX)
            copy = pltpu.make_async_remote_copy(
                src_ref=part_ref.at[pl.ds(pl.multiple_of((zp * NX + xp) * per, per), per)],
                dst_ref=recvx.at[n, o - 1],
                send_sem=sx.at[n, o - 1],
                recv_sem=rx.at[n, o - 1],
                device_id=(zi * NX + xp, cand, dp),
                device_id_type=MESH,
            )
            copy.start()
            row.append(copy)
        xcopies.append(row)

    tower(PLAN[1])

    zcopies = []
    pooled = None
    for n, k in enumerate(turns):
        zp = beside[k]
        for copy in xcopies[n]:
            copy.wait_recv()
        mine = part_ref[pl.ds(pl.multiple_of((zp * NX + xi) * per, per), per), :]
        total = mine + recvx[n, 0] + recvx[n, 1] + recvx[n, 2]
        if k == 0:
            pooled = total
        else:
            sendz[k - 1] = total
            copy = pltpu.make_async_remote_copy(
                src_ref=sendz.at[k - 1],
                dst_ref=recvz.at[k - 1],
                send_sem=sz.at[k - 1],
                recv_sem=rz.at[k - 1],
                device_id=(zp * NX + xi, cand, dp),
                device_id_type=MESH,
            )
            copy.start()
            zcopies.append(copy)
    if PLAN[2]:
        tower(PLAN[2])
    loads[3].wait()
    for copy in zcopies:
        copy.wait_recv()
    pooled = pooled + recvz[0] + recvz[1] + recvz[2]

    p0 = pooled.astype(bf16)
    rest = pooled - p0.astype(f32)
    p1 = rest.astype(bf16)
    p2 = (rest - p1.astype(f32)).astype(bf16)
    terms = jnp.dot(jnp.concatenate([p0, p1, p2], axis=0), wv[...], preferred_element_type=f32)
    terms = terms[:per] + terms[per : 2 * per] + terms[2 * per :]
    for b in range(groups):
        sendt[b] = terms[b * own : (b + 1) * own, :]

    for k in (2, 1, 3, 0):
        for a in range(ncand):
            that = lax.rem(dp + k, ndp)
            holder = lax.rem((a // 2) * NZ + zi + (2 if a % 2 else ring - 2), ring)
            pltpu.make_async_remote_copy(
                src_ref=sendt.at[a * ndp + that],
                dst_ref=recvt.at[table],
                send_sem=st,
                recv_sem=rt,
                device_id=(opposite, lax.div(holder, NZ) * 2 + a % 2, that),
                device_id_type=MESH,
            ).start()

    tower(PLAN[3])
    all_t = pltpu.make_async_copy(recvt, recvt, rt)
    all_t.wait()
    total = recvt[0]
    for b in range(1, groups):
        total = total + recvt[b]
    embed = unit_rows(total)
    embed_ref[...] = embed

    me = tab * ndp + dp

    for away in (2 + 4 * core, 1, ring - 1, 0):
        zq = lax.rem(zring + away, ring)
        zp = lax.rem(zq, NZ)
        share = lax.div(zq, NZ) * 2 + core
        same = isinstance(away, int) and away == 0

        @pl.loop(1 if same else 0, NX * ndp, unroll=5 if same else 4)
        def _(n):
            xp = lax.rem(xi + lax.div(n, ndp), NX)
            pltpu.make_async_remote_copy(
                src_ref=embed_ref,
                dst_ref=gathered.at[me],
                send_sem=sg,
                recv_sem=rg.at[lax.rem(lax.div(zp, 2) + lax.div(zi, 2), 2)],
                device_id=(zp * NX + xp, share, lax.rem(dp + n, ndp)),
                device_id_type=MESH,
            ).start()

    gathered[me] = embed
    tower(PLAN[4])
    lines = place_ref.shape[0]
    half = ntab * ndp // 2

    def add_scores(side, first):
        pieces = [gathered[side * half + b] for b in range(half)]
        items = jnp.concatenate(pieces, axis=0)
        item_high, item_low = split2(items)
        count = items.shape[0]
        stacked = jnp.concatenate([item_high, item_low], axis=0)

        def score(c, _):
            at = pl.ds(pl.multiple_of(c * USERS_AT_ONCE, USERS_AT_ONCE), USERS_AT_ONCE)
            both = jnp.dot(stacked, high_ref[:, at], preferred_element_type=f32)
            rest = jnp.dot(item_high, low_ref[:, at], preferred_element_type=f32)
            scores = both[:count] + both[count:] + rest
            sums = jnp.sum(jnp.exp(scores), axis=0, keepdims=True)
            for h in range(USERS_AT_ONCE // 128):
                line = c * (USERS_AT_ONCE // 128) + h
                place = place_ref[pl.ds(line, 1), :]
                block = lax.shift_right_logical(place, 4)
                apart = (lax.shift_right_logical(block, 4) + 2 - zi) & (NZ - 1)
                apart = jnp.where(apart == 3, ring - 1, jnp.where(apart == 2, 6 - 4 * core, apart))
                owner = (zring + apart + 2 + 4 * core) & (ring - 1)
                here = (block & 3) == lax.shift_right_logical(owner, 2) * 2 + core
                slot = (lax.shift_right_logical(block, 2) + 2 * NX) & (ntab - 1)
                row = jnp.where(here, slot * 16 + (place & 15) - side * count, -1)
                part = scores[:, h * 128 : (h + 1) * 128]
                positive = jnp.sum(
                    jnp.where(iota((count, 128), 0) == row, part, f32(0.0)), axis=0, keepdims=True
                )
                total = sums[:, h * 128 : (h + 1) * 128]
                if not first:
                    total = total + stats[pl.ds(line, 1), :]
                    positive = positive + stats[pl.ds(line + lines, 1), :]
                stats[pl.ds(line, 1), :] = total
                stats[pl.ds(line + lines, 1), :] = positive
            return 0

        lax.fori_loop(0, high_ref.shape[1] // USERS_AT_ONCE, score, 0, unroll=UNROLL)

    most = gathered.at[pl.ds(0, ntab * ndp - 1)]
    near = gathered.at[pl.ds(0, half - 1)]
    far = gathered.at[pl.ds(0, half)]
    side = lax.div(zi, 2)
    pltpu.make_async_copy(near, near, rg.at[0]).wait()
    add_scores(side, True)
    pltpu.make_async_copy(far, far, rg.at[1]).wait()
    item_ref[...] = gathered[opposite * ndp + dp]
    add_scores(1 - side, False)

    scopies = []
    for o in range(1, ncand):
        copy = pltpu.make_async_remote_copy(
            src_ref=stats,
            dst_ref=others.at[o - 1],
            send_sem=ss.at[o - 1],
            recv_sem=rs.at[o - 1],
            device_id=(tab, lax.rem(cand + o, ncand), dp),
            device_id_type=MESH,
        )
        copy.start()
        scopies.append(copy)
    for row in xcopies:
        for copy in row:
            copy.wait_send()
    for copy in zcopies:
        copy.wait_send()
    pltpu.make_async_copy(recvt, recvt, st).wait()
    pltpu.make_async_copy(most, most, sg).wait()
    for copy in scopies:
        copy.wait_recv()
    both = stats[...] + others[0] + others[1] + others[2]
    loss_ref[...] = jnp.log(both[:lines]) - both[lines:]
    for copy in scopies:
        copy.wait_send()


def step(flat, extra, lengths, table, item_weight, features, user_w1, user_w2, places):
    items, width = extra.shape
    rows = table.shape[0]
    users, features_in = features.shape
    hidden, embed = user_w2.shape
    per = items // (NX * NZ)
    own = per // 16
    lines = users // 128
    vmem = pl.BlockSpec(memory_space=pltpu.VMEM)
    hbm = pl.BlockSpec(memory_space=pltpu.HBM)
    dma = pltpu.SemaphoreType.DMA
    return pl.pallas_call(
        step_kernel,
        name="step",
        out_shape=(jax.ShapeDtypeStruct((own, embed), f32), jax.ShapeDtypeStruct((lines, 128), f32)),
        in_specs=[vmem, vmem, vmem, hbm, hbm, hbm, hbm, hbm, vmem],
        out_specs=(vmem, vmem),
        scratch_shapes=[
            pltpu.VMEM((rows, width), bf16),
            pltpu.VMEM((rows, width), f32),
            pltpu.VMEM((128 * LINES, width), f32),
            pltpu.VMEM((items, width), f32),
            pltpu.VMEM((items, width), f32),
            pltpu.VMEM((users, features_in), bf16),
            pltpu.VMEM((features_in, hidden), bf16),
            pltpu.VMEM((hidden, embed), bf16),
            pltpu.VMEM((width, embed), bf16),
            pltpu.VMEM((embed, users), bf16),
            pltpu.VMEM((embed, users), bf16),
            pltpu.VMEM((NZ, NX - 1, per, width), f32),
            pltpu.VMEM((NZ - 1, per, width), f32),
            pltpu.VMEM((NZ - 1, per, width), f32),
            pltpu.VMEM((16, own, embed), f32),
            pltpu.VMEM((16, own, embed), f32),
            pltpu.VMEM((own, embed), f32),
            pltpu.VMEM((64, own, embed), f32),
            pltpu.VMEM((2 * lines, 128), f32),
            pltpu.VMEM((3, 2 * lines, 128), f32),
            pltpu.SMEM((8, 128), i32),
            dma,
            dma((CHUNKS,)),
            dma((4,)),
            dma((NZ, NX - 1)),
            dma((NZ, NX - 1)),
            dma((NZ - 1,)),
            dma((NZ - 1,)),
            dma,
            dma,
            dma,
            dma((2,)),
            dma((3,)),
            dma((3,)),
        ],
        compiler_params=pltpu.CompilerParams(
            collective_id=0, has_side_effects=True, vmem_limit_bytes=52 * 2**20
        ),
        cost_estimate=pl.CostEstimate(flops=5 * 10**9, bytes_accessed=5 * 2**20, transcendentals=0),
    )(flat, extra, lengths, table, item_weight, features, user_w1, user_w2, places)


def finish_kernel(item_ref, loss_ref, item_out, loss_out):
    item_out[...] = item_ref[...]
    loss_out[...] = loss_ref[...]


def finish(item_emb, loss):
    vmem = pl.BlockSpec(memory_space=pltpu.VMEM)
    return pl.pallas_call(
        finish_kernel,
        name="finish",
        out_shape=(
            jax.ShapeDtypeStruct(item_emb.shape, f32),
            jax.ShapeDtypeStruct(loss.shape, f32),
        ),
        in_specs=[vmem, vmem],
        out_specs=(vmem, vmem),
        compiler_params=pltpu.CompilerParams(vmem_limit_bytes=2**20),
    )(item_emb, loss)


def body(
    tables, bag_ids, bag_lengths, item_weight, user_features, user_w1, user_w2, positive_items
):
    ids = bag_ids[0].T
    ids = jnp.where(iota(ids.shape, 0) < bag_lengths, ids, i32(-1))
    flat, extra = make_list(ids, tables[0])
    item_emb, loss = step(
        flat, extra, bag_lengths, tables[0], item_weight, user_features, user_w1, user_w2, positive_items.reshape(-1, 128)
    )
    item_emb, loss = finish(item_emb, loss)
    return (item_emb, loss.reshape(-1))


def solution(mesh):
    placed = (
        P(("cand", "dp"), "tab", None),
        P(("cand", "dp"), None, None),
        P(("cand", "dp"), None),
        P(),
        P(("tab", "dp"), None),
        P(),
        P(),
        P(("tab", "dp")),
    )
    return jax.shard_map(
        body,
        mesh=mesh,
        in_specs=placed,
        out_specs=(P(("tab", "cand", "dp"), None), P(("tab", "dp"))),
        check_vma=False,
    )
```
